128 devices in a mesh: batch: 1, outer: 16 (over z, y), rows: 8 (over x, core).
Axes of the slice: x: 4, y: 4, z: 4, core: 2. Of those that a mesh axis runs over, the one named last changes fastest.
Arguments:
- a_mat: float32 [131072, 896], P(('batch', 'outer', 'rows'))
Outputs:
- output 1: float32 [131072, 896], P(('batch', 'outer', 'rows'))
- output 2: float32 [896, 896], P('batch')
All inputs are finite; a program needn't handle non-finite values.
Results may differ from the reference program's by a relative error of at most 0.001.
Values sent between devices are 32-bit elements.
A program may use at most 1 GiB of HBM per device.

```python
import jax
import jax.numpy as jnp
from jax import lax

TOTAL_ROWS = 131072
N_COLS = 896


def gram_of(row_blk):
    return lax.dot_general(row_blk, row_blk, (((0,), (0,)), ((), ())), precision=lax.Precision.HIGHEST, preferred_element_type=jnp.float32)


def chol_sweep(row_blk):
    low_fac = jnp.linalg.cholesky(gram_of(row_blk))
    solved = lax.linalg.triangular_solve(low_fac, row_blk, left_side=False, lower=True, transpose_a=True)
    return solved, low_fac


def setup_inputs(seed: int = 0, part: int = 0) -> dict:
    key = jax.random.fold_in(jax.random.key(seed), part)
    key_rows, key_mix = jax.random.split(key)
    base_rows = jax.random.normal(key_rows, (TOTAL_ROWS, N_COLS), jnp.float32)
    ortho_mix = jnp.linalg.qr(jax.random.normal(key_mix, (N_COLS, N_COLS), jnp.float32))[0]
    col_idx = jnp.arange(N_COLS, dtype=jnp.float32)
    spectrum = jnp.power(10.0, -3.0 * col_idx / (N_COLS - 1))
    mixing = spectrum[:, None] * ortho_mix.T
    a_mat = jnp.dot(base_rows, mixing, precision=lax.Precision.HIGHEST, preferred_element_type=jnp.float32)
    return {"a_mat": a_mat}


def reference(a_mat):
    q_one, low_one = chol_sweep(a_mat)
    q_two, low_two = chol_sweep(q_one)
    r_fac = lax.dot_general(low_two, low_one, (((0,), (1,)), ((), ())), precision=lax.Precision.HIGHEST, preferred_element_type=jnp.float32)
    return q_two, r_fac
```

```python
import functools
import jax, jax.numpy as jnp
from jax import lax
from jax.experimental import pallas as pl
from jax.experimental.pallas import tpu as pltpu

HI = lax.Precision.HIGHEST
N = 896
B = 128
NB = N // B


def dot(a, b, ca, cb):
    return lax.dot_general(a, b, (((ca,), (cb,)), ((), ())), precision=HI, preferred_element_type=jnp.float32)


def factor_diag(diag):
    ng = B // 8
    sub = lax.broadcasted_iota(jnp.int32, (8, B), 0)
    lane = lax.broadcasted_iota(jnp.int32, (8, B), 1)
    rows = list(diag)
    inv = [jnp.where(lane == sub + 8 * q, 1.0, 0.0).astype(jnp.float32) for q in range(ng)]
    for p in range(ng):
        cols = [jnp.broadcast_to(rows[p][:, 8 * p + k:8 * p + k + 1], (8, B)) for k in range(8)]
        u = [None] * 8
        ux = [None] * 8
        rec = [None] * 8
        cross = {}
        scale = jnp.zeros((8, B), jnp.float32)
        dp, xp = rows[p], inv[p]
        for k in range(8):
            piv = jnp.broadcast_to(cols[k][k:k + 1, :], (8, B))
            rec[k] = 1.0 / piv
            scale = jnp.where(sub == k, piv, scale)
            low = jnp.where(sub > k, cols[k] * rec[k], 0.0)
            u[k] = jnp.broadcast_to(dp[k:k + 1, :], (8, B))
            ux[k] = jnp.broadcast_to(xp[k:k + 1, :], (8, B))
            for kk in range(k + 1, 8):
                cross[k, kk] = jnp.broadcast_to(cols[kk][k:k + 1, :], (8, B))
                cols[kk] = cols[kk] - low * cross[k, kk]
            dp = dp - low * u[k]
            xp = xp - low * ux[k]
        rs = lax.rsqrt(scale)
        rows[p] = dp * rs
        inv[p] = xp * rs
        for q in range(p + 1, ng):
            cq = [jnp.broadcast_to(rows[q][:, 8 * p + k:8 * p + k + 1], (8, B)) for k in range(8)]
            dq, xq = rows[q], inv[q]
            for k in range(8):
                low = cq[k] * rec[k]
                for kk in range(k + 1, 8):
                    cq[kk] = cq[kk] - low * cross[k, kk]
                dq = dq - low * u[k]
                xq = xq - low * ux[k]
            rows[q], inv[q] = dq, xq
    for q in range(ng):
        rows[q] = jnp.where(lane >= sub + 8 * q, rows[q], 0.0)
    return rows, inv


def chol_kernel(g_ref, r_ref, x_ref, w, xd):
    ng = B // 8
    w[:, :N] = g_ref[...]
    w[:, N:] = jnp.zeros((N, N), jnp.float32)

    def step(j, _):
        r0 = pl.multiple_of(j * B, B)
        rr = pl.ds(r0, B)
        diag = [w[pl.ds(pl.multiple_of(r0 + 8 * q, 8), 8), pl.ds(r0, B)] for q in range(ng)]
        rows, inv = factor_diag(diag)
        for q in range(ng):
            w[pl.ds(pl.multiple_of(r0 + 8 * q, 8), 8), pl.ds(r0, B)] = rows[q]
            w[pl.ds(pl.multiple_of(r0 + 8 * q, 8), 8), pl.ds(pl.multiple_of(r0 + N, B), B)] = inv[q]
            xd[pl.ds(8 * q, 8), :] = inv[q]
        mid = pl.ds(pl.multiple_of(r0 + B, B), N - B)
        w[rr, mid] = dot(xd[...], w[rr, mid], 1, 0)
        win = pl.ds(pl.multiple_of(r0 + B, B), N)

        def trail(i, _):
            ri = pl.ds(pl.multiple_of(i * B, B), B)
            left = w[rr, ri]
            w[ri, win] = w[ri, win] - dot(left, w[rr, win], 0, 0)
            return 0

        lax.fori_loop(j + 1, NB, trail, 0)
        return 0

    lax.fori_loop(0, NB, step, 0)
    for i in range(NB):
        ri = pl.ds(i * B, B)
        if i:
            r_ref[ri, :i * B] = jnp.zeros((B, i * B), jnp.float32)
        r_ref[ri, i * B:] = w[ri, i * B:N]
        x_ref[ri, :(i + 1) * B] = w[ri, N:N + (i + 1) * B]
        if i < NB - 1:
            x_ref[ri, (i + 1) * B:] = jnp.zeros((B, N - (i + 1) * B), jnp.float32)


def chol_inv(g):
    return pl.pallas_call(
        chol_kernel,
        out_shape=[jax.ShapeDtypeStruct((N, N), jnp.float32)] * 2,
        in_specs=[pl.BlockSpec(memory_space=pltpu.VMEM)],
        out_specs=[pl.BlockSpec(memory_space=pltpu.VMEM)] * 2,
        scratch_shapes=[pltpu.VMEM((N, 2 * N), jnp.float32), pltpu.VMEM((B, B), jnp.float32)],
        compiler_params=pltpu.CompilerParams(vmem_limit_bytes=56 * 2**20),
        name="chol_inv",
    )(g)


GROUP_AXES = ("outer", "rows")


def solution(mesh):
    from jax.sharding import PartitionSpec as P
    row_spec = P(("batch", "outer", "rows"), None)

    def local_qr(a):
        g1 = lax.psum(dot(a, a, 0, 0), GROUP_AXES)
        r1, x1 = chol_inv(g1)
        q1 = dot(a, x1, 1, 1)
        g2 = lax.psum(dot(q1, q1, 0, 0), GROUP_AXES)
        r2, x2 = chol_inv(g2)
        return dot(q1, x2, 1, 1), dot(r2, r1, 1, 0)

    return jax.shard_map(local_qr, mesh=mesh, in_specs=(row_spec,), out_specs=(row_spec, P("batch", None)), check_vma=False)
```

```python
import jax, jax.numpy as jnp
from jax import lax
from jax.experimental import pallas as pl
from jax.experimental.pallas import tpu as pltpu
from jax.sharding import PartitionSpec as P

HI = lax.Precision.HIGHEST
N = 896
B = 128
NB = N // B


def dot(a, b, ca, cb):
    return lax.dot_general(a, b, (((ca,), (cb,)), ((), ())), precision=HI, preferred_element_type=jnp.float32)


def factor_diag(diag):
    ng = B // 8
    sub = lax.broadcasted_iota(jnp.int32, (8, B), 0)
    lane = lax.broadcasted_iota(jnp.int32, (8, B), 1)
    rows = list(diag)
    inv = [jnp.where(lane == sub + 8 * q, 1.0, 0.0).astype(jnp.float32) for q in range(ng)]
    for p in range(ng):
        cols = [jnp.broadcast_to(rows[p][:, 8 * p + k:8 * p + k + 1], (8, B)) for k in range(8)]
        u = [None] * 8
        ux = [None] * 8
        rec = [None] * 8
        cross = {}
        scale = jnp.zeros((8, B), jnp.float32)
        dp, xp = rows[p], inv[p]
        for k in range(8):
            piv = jnp.broadcast_to(cols[k][k:k + 1, :], (8, B))
            rec[k] = 1.0 / piv
            scale = jnp.where(sub == k, piv, scale)
            low = jnp.where(sub > k, cols[k] * rec[k], 0.0)
            u[k] = jnp.broadcast_to(dp[k:k + 1, :], (8, B))
            ux[k] = jnp.broadcast_to(xp[k:k + 1, :], (8, B))
            for kk in range(k + 1, 8):
                cross[k, kk] = jnp.broadcast_to(cols[kk][k:k + 1, :], (8, B))
                cols[kk] = cols[kk] - low * cross[k, kk]
            dp = dp - low * u[k]
            xp = xp - low * ux[k]
        rs = lax.rsqrt(scale)
        rows[p] = dp * rs
        inv[p] = xp * rs
        for q in range(p + 1, ng):
            cq = [jnp.broadcast_to(rows[q][:, 8 * p + k:8 * p + k + 1], (8, B)) for k in range(8)]
            dq, xq = rows[q], inv[q]
            for k in range(8):
                low = cq[k] * rec[k]
                for kk in range(k + 1, 8):
                    cq[kk] = cq[kk] - low * cross[k, kk]
                dq = dq - low * u[k]
                xq = xq - low * ux[k]
            rows[q], inv[q] = dq, xq
    for q in range(ng):
        rows[q] = jnp.where(lane >= sub + 8 * q, rows[q], 0.0)
    return rows, inv


def chol_kernel(g_ref, r_ref, x_ref, w, xd):
    ng = B // 8
    w[...] = jnp.zeros((N, 2 * N), jnp.float32)
    for i in range(NB):
        for j in range(i, NB):
            w[i * B:(i + 1) * B, j * B:(j + 1) * B] = g_ref[pl.ds(block_row(i, j), B), :]

    def step(j, _):
        r0 = pl.multiple_of(j * B, B)
        rr = pl.ds(r0, B)
        diag = [w[pl.ds(pl.multiple_of(r0 + 8 * q, 8), 8), pl.ds(r0, B)] for q in range(ng)]
        rows, inv = factor_diag(diag)
        for q in range(ng):
            w[pl.ds(pl.multiple_of(r0 + 8 * q, 8), 8), pl.ds(r0, B)] = rows[q]
            w[pl.ds(pl.multiple_of(r0 + 8 * q, 8), 8), pl.ds(pl.multiple_of(r0 + N, B), B)] = inv[q]
            xd[pl.ds(8 * q, 8), :] = inv[q]
        mid = pl.ds(pl.multiple_of(r0 + B, B), N - B)
        w[rr, mid] = dot(xd[...], w[rr, mid], 1, 0)
        win = pl.ds(pl.multiple_of(r0 + B, B), N)

        def trail(i, _):
            ri = pl.ds(pl.multiple_of(i * B, B), B)
            left = w[rr, ri]
            w[ri, win] = w[ri, win] - dot(left, w[rr, win], 0, 0)
            return 0

        lax.fori_loop(j + 1, NB, trail, 0)
        return 0

    lax.fori_loop(0, NB, step, 0)
    for i in range(NB):
        ri = pl.ds(i * B, B)
        if i:
            r_ref[ri, :i * B] = jnp.zeros((B, i * B), jnp.float32)
        r_ref[ri, i * B:] = w[ri, i * B:N]
        x_ref[ri, :(i + 1) * B] = w[ri, N:N + (i + 1) * B]
        if i < NB - 1:
            x_ref[ri, (i + 1) * B:] = jnp.zeros((B, N - (i + 1) * B), jnp.float32)


def chol_inv(g):
    return pl.pallas_call(
        chol_kernel,
        out_shape=[jax.ShapeDtypeStruct((N, N), jnp.float32)] * 2,
        in_specs=[pl.BlockSpec(memory_space=pltpu.VMEM)],
        out_specs=[pl.BlockSpec(memory_space=pltpu.VMEM)] * 2,
        scratch_shapes=[pltpu.VMEM((N, 2 * N), jnp.float32), pltpu.VMEM((B, B), jnp.float32)],
        compiler_params=pltpu.CompilerParams(vmem_limit_bytes=56 * 2**20),
        name="chol_inv",
    )(g)


CH = 32
PIECE = 8 * CH
HALF = 8 * PIECE
ROWS_PACKED = 2 * HALF
MESH_T = pl.DeviceIdType.MESH
ORDER = (7, 3, 5, 6, 1, 2, 4)


def _bits(d):
    return tuple((d >> s) & 1 for s in range(3))


def _flip(v, kind):
    return (1 - kind) * (v + 1 - 2 * (v % 2)) + kind * (3 - v)


def _label(v, kind):
    return (1 - kind) * ((v % 2 + v // 2) % 2) + kind * (v // 2)


def ar_kernel(p_ref, o_ref, rec0, acc0, rec1, acc1, rec2, s0, t0, s1, t1, s2, t2, s3, t3, s4, t4, s5, t5):
    outer, row = lax.axis_index("outer"), lax.axis_index("rows")
    pos = (row // 2, outer % 4, outer // 4)
    core = row % 2
    kinds = (core, 1 - core)
    labels = [tuple(_label(v, k) for v in pos) for k in kinds]

    def peer(stage, d):
        x, y, z = (_flip(v, kinds[stage]) if b else v for v, b in zip(pos, _bits(d)))
        return {"outer": z * 4 + y, "rows": x * 2 + core}

    def index(stage, d):
        return sum((1 - v if b else v) * (1 << s) for s, (v, b) in enumerate(zip(labels[stage], _bits(d))))

    partner = {"outer": outer, "rows": pos[0] * 2 + 1 - core}
    everyone = [partner] + [peer(s, d) for s in range(2) for d in range(1, 8)]

    barrier = pltpu.get_barrier_semaphore()
    for dev in everyone:
        pl.semaphore_signal(barrier, inc=1, device_id=dev, device_id_type=MESH_T)
    pl.semaphore_wait(barrier, len(everyone))

    def copy(src, dst, send, recv, dev):
        return pltpu.make_async_remote_copy(src_ref=src, dst_ref=dst, send_sem=send, recv_sem=recv, device_id=dev, device_id_type=MESH_T)

    def piece(half, i):
        return pl.ds(pl.multiple_of(half * HALF + i * PIECE, PIECE), PIECE)

    sent = []

    def go(c):
        c.start()
        sent.append(c)
        return c

    first = [go(copy(p_ref.at[piece(1 - core, index(1, d))], rec0.at[d], s0.at[d], t0.at[d], partner)) for d in ORDER + (0,)]
    out1 = {}
    for n, d in enumerate(ORDER + (0,)):
        first[n].wait_recv()
        acc0[d] = p_ref[piece(core, index(0, d)), :] + rec0[d]
        if d:
            out1[d] = go(copy(acc0.at[d], rec1.at[d - 1], s1.at[d - 1], t1.at[d - 1], peer(0, d)))
    for d in range(1, 8):
        out1[d].wait_recv()
    total = acc0[0]
    for d in range(1, 8):
        total = total + rec1[d - 1]
    acc1[...] = total
    out2 = {}
    for e in ORDER:
        rows = pl.ds(pl.multiple_of(index(1, e) * CH, CH), CH)
        out2[e] = go(copy(acc1.at[rows], rec2.at[e - 1], s2.at[e - 1], t2.at[e - 1], peer(1, e)))
    for e in range(1, 8):
        out2[e].wait_recv()
    total = acc1[pl.ds(pl.multiple_of(index(1, 0) * CH, CH), CH), :]
    for e in range(1, 8):
        total = total + rec2[e - 1]

    def chunk(e):
        return pl.ds(pl.multiple_of(core * HALF + index(0, 0) * PIECE + index(1, e) * CH, CH), CH)

    o_ref[chunk(0), :] = total
    for e in ORDER:
        go(copy(o_ref.at[chunk(0)], o_ref.at[chunk(0)], s3.at[e - 1], t3.at[e - 1], peer(1, e)))
    for e in range(1, 8):
        copy(o_ref.at[chunk(e)], o_ref.at[chunk(e)], s3.at[e - 1], t3.at[e - 1], peer(1, e)).wait_recv()
    mine = piece(core, index(0, 0))
    for d in ORDER:
        go(copy(o_ref.at[mine], o_ref.at[mine], s4.at[d - 1], t4.at[d - 1], peer(0, d)))
    go(copy(o_ref.at[mine], o_ref.at[mine], s5.at[0], t5.at[0], partner))
    for d in (1, 2, 4, 3, 5, 6, 7):
        got = piece(core, index(0, d))
        copy(o_ref.at[got], o_ref.at[got], s4.at[d - 1], t4.at[d - 1], peer(0, d)).wait_recv()
        go(copy(o_ref.at[got], o_ref.at[got], s5.at[d], t5.at[d], partner))
    for d in range(8):
        got = piece(1 - core, index(1, d))
        copy(o_ref.at[got], o_ref.at[got], s5.at[d], t5.at[d], partner).wait_recv()
    for c in sent:
        c.wait_send()


def all_reduce(p, ident):
    sems = []
    for n in (8, 7, 7, 7, 7, 8):
        sems += [pltpu.SemaphoreType.DMA((n,))] * 2
    return pl.pallas_call(
        ar_kernel,
        out_shape=jax.ShapeDtypeStruct((ROWS_PACKED, B), jnp.float32),
        in_specs=[pl.BlockSpec(memory_space=pltpu.VMEM)],
        out_specs=pl.BlockSpec(memory_space=pltpu.VMEM),
        scratch_shapes=[
            pltpu.VMEM((8, PIECE, B), jnp.float32),
            pltpu.VMEM((8, PIECE, B), jnp.float32),
            pltpu.VMEM((7, PIECE, B), jnp.float32),
            pltpu.VMEM((PIECE, B), jnp.float32),
            pltpu.VMEM((7, CH, B), jnp.float32),
        ] + sems,
        compiler_params=pltpu.CompilerParams(collective_id=ident, has_side_effects=True),
        name="sum_group",
    )(p)


M_LOC = 1024
STEP = 256
TILES = [(lo, min(lo + 256, N)) for lo in range(0, N, 256)]


def block_row(i, j):
    return (i * NB - i * (i - 1) // 2 + j - i) * B


def add_gram(rows, p_ref):
    for lo, hi in TILES:
        c = dot(rows[:, :hi], rows[:, lo:hi], 0, 0)
        for j in range(lo // B, hi // B):
            for i in range(j + 1):
                at = pl.ds(block_row(i, j), B)
                p_ref[at, :] = p_ref[at, :] + c[i * B:(i + 1) * B, j * B - lo:(j + 1) * B - lo]


def gram_kernel(a_ref, p_ref):
    p_ref[...] = jnp.zeros(p_ref.shape, jnp.float32)

    def body(s, _):
        add_gram(a_ref.at[pl.ds(pl.multiple_of(s * STEP, STEP), STEP)], p_ref)
        return 0

    lax.fori_loop(0, M_LOC // STEP, body, 0)


def solve_gram_kernel(a_ref, x_ref, q_ref, p_ref):
    p_ref[...] = jnp.zeros(p_ref.shape, jnp.float32)

    def body(s, _):
        at = pl.ds(pl.multiple_of(s * STEP, STEP), STEP)
        for lo, hi in TILES:
            q_ref[at, lo:hi] = dot(a_ref[at, :hi], x_ref[lo:hi, :hi], 1, 1)
        add_gram(q_ref.at[at], p_ref)
        return 0

    lax.fori_loop(0, M_LOC // STEP, body, 0)


def solve_kernel(a_ref, x_ref, r2_ref, r1_ref, q_ref, r_ref):
    def body(s, _):
        at = pl.ds(pl.multiple_of(s * STEP, STEP), STEP)
        for lo, hi in TILES:
            q_ref[at, lo:hi] = dot(a_ref[at, :hi], x_ref[lo:hi, :hi], 1, 1)
        return 0

    lax.fori_loop(0, M_LOC // STEP, body, 0)
    for lo, hi in TILES:
        if lo:
            r_ref[lo:hi, :lo] = jnp.zeros((hi - lo, lo), jnp.float32)
        r_ref[lo:hi, lo:] = dot(r2_ref[lo:hi, lo:], r1_ref[lo:, lo:], 1, 0)


def vm(n):
    return [pl.BlockSpec(memory_space=pltpu.VMEM)] * n


PARAMS = pltpu.CompilerParams(vmem_limit_bytes=56 * 2**20)
F32 = lambda *s: jax.ShapeDtypeStruct(s, jnp.float32)


def gram(a):
    return pl.pallas_call(gram_kernel, out_shape=F32(ROWS_PACKED, B), in_specs=vm(1), out_specs=vm(1)[0], compiler_params=PARAMS, name="gram")(a)


def solve_gram(a, x):
    return pl.pallas_call(solve_gram_kernel, out_shape=[F32(M_LOC, N), F32(ROWS_PACKED, B)], in_specs=vm(2), out_specs=vm(2), compiler_params=PARAMS, name="solve_gram")(a, x)


def solve(a, x, r2, r1):
    return pl.pallas_call(solve_kernel, out_shape=[F32(M_LOC, N), F32(N, N)], in_specs=vm(4), out_specs=vm(2), compiler_params=PARAMS, name="solve")(a, x, r2, r1)


def solution(mesh):
    row_spec = P(("batch", "outer", "rows"), None)

    def local_qr(a):
        r1, x1 = chol_inv(all_reduce(gram(a), 0))
        q1, p2 = solve_gram(a, x1)
        r2, x2 = chol_inv(all_reduce(p2, 1))
        return tuple(solve(q1, x2, r2, r1))

    return jax.shard_map(local_qr, mesh=mesh, in_specs=(row_spec,), out_specs=(row_spec, P("batch", None)), check_vma=False)
```

```python
import jax
import jax.numpy as jnp
from jax import lax
from jax.experimental import pallas as pl
from jax.experimental.pallas import tpu as pltpu
from jax.sharding import PartitionSpec as P

HI = lax.Precision.HIGHEST
N = 896
B = 128
NB = N // B
NG = B // 8


def dot(a, b, ca, cb):
    return lax.dot_general(a, b, (((ca,), (cb,)), ((), ())), precision=HI, preferred_element_type=jnp.float32)


def lane_col(v, c):
    lane = lax.broadcasted_iota(jnp.int32, (8, B), 1)
    return jnp.broadcast_to(jnp.sum(jnp.where(lane == c, v, 0.0), axis=1, keepdims=True), (8, B))


def sub_row(v, k):
    return jnp.broadcast_to(v[k:k + 1, :], (8, B))


def factor_diag(diag):
    sub = lax.broadcasted_iota(jnp.int32, (8, B), 0)
    lane = lax.broadcasted_iota(jnp.int32, (8, B), 1)
    m = list(diag)
    rows, inv = [None] * NG, [None] * NG
    for p in range(NG):
        g0 = 8 * p
        here = (lane >= g0) & (lane < g0 + 8)
        cols = [lane_col(m[p], g0 + k) for k in range(8)]
        z = jnp.where(here, jnp.where(lane == sub + g0, 1.0, 0.0), m[p])
        near = p + 1 < NG
        if near:
            cq = [lane_col(m[p + 1], g0 + k) for k in range(8)]
            mq = jnp.where(here, 0.0, m[p + 1])
        recs = jnp.zeros((8, B), jnp.float32)
        pivs = jnp.ones((8, B), jnp.float32)
        for k in range(8):
            piv = sub_row(cols[k], k)
            rec = 1.0 / piv
            pivs = jnp.where(sub == k, piv, pivs)
            recs = jnp.where(sub == k, rec, recs)
            low = jnp.where(sub > k, cols[k] * rec, 0.0)
            for kk in range(k + 1, 8):
                cross = sub_row(cols[kk], k)
                cols[kk] = cols[kk] - low * cross
                if near:
                    if kk == k + 1:
                        lq = cq[k] * rec
                    cq[kk] = cq[kk] - lq * cross
            if near and k == 7:
                lq = cq[k] * rec
            uz = sub_row(z, k)
            z = z - low * uz
            if near:
                mq = mq - lq * uz
        scale = lax.rsqrt(pivs)
        upper = z
        for kk in range(8):
            upper = jnp.where(lane == g0 + kk, cols[kk], upper)
        rows[p] = jnp.where(lane >= sub + g0, upper * scale, 0.0)
        inv[p] = jnp.where(lane < g0 + 8, z * scale, 0.0)
        if p + 2 < NG:
            wv = z * recs
            for kk in range(7, 0, -1):
                wv = wv - jnp.where(sub < kk, cols[kk] * recs, 0.0) * sub_row(wv, kk)
            wk = [sub_row(wv, k) for k in range(8)]
            for q in range(p + 2, NG):
                new = jnp.where(here, 0.0, m[q])
                for k in range(8):
                    new = new - lane_col(m[q], g0 + k) * wk[k]
                m[q] = new
        if near:
            m[p + 1] = mq
    return rows, inv


def block_row(i, j):
    return (i * NB - i * (i - 1) // 2 + j - i) * B


def mult(x):
    return pl.multiple_of(x, B)


def factor(g_ref, w, xd):
    w[:, N:] = jnp.zeros((N, N), jnp.float32)
    for i in range(NB):
        for j in range(i):
            w[i * B:(i + 1) * B, j * B:(j + 1) * B] = jnp.zeros((B, B), jnp.float32)
        for j in range(i, NB):
            w[i * B:(i + 1) * B, j * B:(j + 1) * B] = g_ref[pl.ds(block_row(i, j), B), :]

    def step(j, _):
        r0 = mult(j * B)
        rr = pl.ds(r0, B)
        group = [pl.ds(pl.multiple_of(r0 + 8 * q, 8), 8) for q in range(NG)]
        rows, inv = factor_diag([w[gq, pl.ds(r0, B)] for gq in group])
        for q in range(NG):
            w[group[q], pl.ds(r0, B)] = rows[q]
            w[group[q], pl.ds(mult(r0 + N), B)] = inv[q]
            xd[pl.ds(8 * q, 8), :] = inv[q]
        mid = pl.ds(mult(r0 + B), N - B)
        w[rr, mid] = dot(xd[...], w[rr, mid], 1, 0)
        odd = j % 2

        def trail(top, depth):
            src = pl.ds(mult(top), depth)
            win = pl.ds(mult(top + depth), N)

            def body(i, _):
                ri = pl.ds(mult(i * B), B)
                w[ri, win] = w[ri, win] - dot(w[src, ri], w[src, win], 0, 0)
                return 0

            return body

        lax.fori_loop(j + 1, jnp.where(odd == 0, jnp.minimum(j + 2, NB), j + 1), trail(r0, B), 0)
        lax.fori_loop(jnp.where(odd == 1, j + 1, NB), NB, trail(jnp.maximum(r0 - B, 0), 2 * B), 0)
        return 0

    lax.fori_loop(0, NB, step, 0)
    for i in range(1, NB):
        w[i * B:(i + 1) * B, :i * B] = jnp.zeros((B, i * B), jnp.float32)


M_LOC = 1024
STEP = 256
NSTEP = M_LOC // STEP
TILES = [(lo, min(lo + 256, N)) for lo in range(0, N, 256)]


def add_gram(rows, p_ref):
    for lo, hi in TILES:
        c = dot(rows[:, :hi], rows[:, lo:hi], 0, 0)
        for j in range(lo // B, hi // B):
            for i in range(j + 1):
                at = pl.ds(block_row(i, j), B)
                p_ref[at, :] = p_ref[at, :] + c[i * B:(i + 1) * B, j * B - lo:(j + 1) * B - lo]


def solve_rows(a, w, q):
    for lo, hi in TILES:
        q[:, lo:hi] = dot(a[:, :hi], w[lo:hi, N:N + hi], 1, 1)


def rows_at(s):
    return pl.ds(pl.multiple_of(s * STEP, STEP), STEP)


def gram_kernel(a_hbm, p_ref, a, sem):
    loads = [pltpu.make_async_copy(a_hbm.at[rows_at(s)], a.at[rows_at(s)], sem.at[s]) for s in range(NSTEP)]
    for c in loads:
        c.start()
    p_ref[...] = jnp.zeros(p_ref.shape, jnp.float32)

    def body(s, _):
        pltpu.make_async_copy(a_hbm.at[rows_at(s)], a.at[rows_at(s)], sem.at[s]).wait()
        add_gram(a.at[rows_at(s)], p_ref)
        return 0

    lax.fori_loop(0, NSTEP, body, 0)


def sweep_one_kernel(g_ref, a_hbm, q_hbm, p_ref, r_hbm, w, xd, a, q, sem, qsem):
    load = pltpu.make_async_copy(a_hbm, a, sem.at[0])
    load.start()
    p_ref[...] = jnp.zeros(p_ref.shape, jnp.float32)
    factor(g_ref, w, xd)
    keep = pltpu.make_async_copy(w.at[:, pl.ds(0, N)], r_hbm, sem.at[1])
    keep.start()
    load.wait()

    def body(s, _):
        at = rows_at(s)
        solve_rows(a.at[at], w, q.at[at])
        pltpu.make_async_copy(q.at[at], q_hbm.at[at], qsem.at[s]).start()
        add_gram(q.at[at], p_ref)
        return 0

    lax.fori_loop(0, NSTEP, body, 0)
    for s in range(NSTEP):
        pltpu.make_async_copy(q.at[rows_at(s)], q_hbm.at[rows_at(s)], qsem.at[s]).wait()
    keep.wait()


def sweep_two_kernel(g_ref, a_hbm, r1_hbm, q_hbm, r_hbm, w, xd, a, q, r1, r, sem, qsem, rsem):
    load = pltpu.make_async_copy(a_hbm, a, sem.at[0])
    load.start()
    load_r = pltpu.make_async_copy(r1_hbm, r1, sem.at[1])
    load_r.start()
    factor(g_ref, w, xd)
    load.wait()

    def body(s, _):
        at = rows_at(s)
        solve_rows(a.at[at], w, q.at[at])
        pltpu.make_async_copy(q.at[at], q_hbm.at[at], qsem.at[s]).start()
        return 0

    lax.fori_loop(0, NSTEP, body, 0)
    load_r.wait()
    stores = []
    for n, (lo, hi) in enumerate(TILES):
        if lo:
            r[lo:hi, :lo] = jnp.zeros((hi - lo, lo), jnp.float32)
        for clo, chi in TILES[n:]:
            r[lo:hi, clo:chi] = dot(w[lo:hi, lo:chi], r1[lo:chi, clo:chi], 1, 0)
        at = pl.ds(lo, hi - lo)
        stores.append(pltpu.make_async_copy(r.at[at], r_hbm.at[at], rsem.at[n]))
        stores[-1].start()
    for s in range(NSTEP):
        pltpu.make_async_copy(q.at[rows_at(s)], q_hbm.at[rows_at(s)], qsem.at[s]).wait()
    for c in stores:
        c.wait()


VM = pl.BlockSpec(memory_space=pltpu.VMEM)
ANY = pl.BlockSpec(memory_space=pl.ANY)
PARAMS = pltpu.CompilerParams(vmem_limit_bytes=58 * 2**20)
DMA = pltpu.SemaphoreType.DMA


def out(*s):
    return jax.ShapeDtypeStruct(s, jnp.float32)


def buf(*s):
    return pltpu.VMEM(s, jnp.float32)


def gram(a):
    return pl.pallas_call(
        gram_kernel, out_shape=out(ROWS_PACKED, B), in_specs=[ANY], out_specs=VM, name="gram",
        scratch_shapes=[buf(M_LOC, N), DMA((NSTEP,))], compiler_params=PARAMS,
    )(a)


def sweep_one(g, a):
    return pl.pallas_call(
        sweep_one_kernel, out_shape=[out(M_LOC, N), out(ROWS_PACKED, B), out(N, N)], in_specs=[VM, ANY], out_specs=[ANY, VM, ANY],
        scratch_shapes=[buf(N, 2 * N), buf(B, B), buf(M_LOC, N), buf(M_LOC, N), DMA((2,)), DMA((NSTEP,))],
        compiler_params=PARAMS, name="sweep_one",
    )(g, a)


def sweep_two(g, q1, r1):
    return pl.pallas_call(
        sweep_two_kernel, out_shape=[out(M_LOC, N), out(N, N)], in_specs=[VM, ANY, ANY], out_specs=[ANY, ANY],
        scratch_shapes=[buf(N, 2 * N), buf(B, B), buf(M_LOC, N), buf(M_LOC, N), buf(N, N), buf(N, N), DMA((2,)), DMA((NSTEP,)), DMA((4,))],
        compiler_params=PARAMS, name="sweep_two",
    )(g, q1, r1)


CH = 32
PIECE = 8 * CH
HALF = 8 * PIECE
ROWS_PACKED = 2 * HALF
MESH_T = pl.DeviceIdType.MESH
ORDER = (7, 3, 5, 6, 1, 2, 4)


def _bits(d):
    return tuple((d >> s) & 1 for s in range(3))


def _flip(v, kind):
    return (1 - kind) * (v + 1 - 2 * (v % 2)) + kind * (3 - v)


def _label(v, kind):
    return (1 - kind) * ((v % 2 + v // 2) % 2) + kind * (v // 2)


def ar_kernel(p_ref, o_ref, rec0, acc0, rec1, acc1, rec2, s0, t0, s1, t1, s2, t2, s3, t3, s4, t4, s5, t5):
    outer, row = lax.axis_index("outer"), lax.axis_index("rows")
    pos = (row // 2, outer % 4, outer // 4)
    core = row % 2
    kinds = (core, 1 - core)
    labels = [tuple(_label(v, k) for v in pos) for k in kinds]

    def peer(stage, d):
        x, y, z = (_flip(v, kinds[stage]) if b else v for v, b in zip(pos, _bits(d)))
        return {"outer": z * 4 + y, "rows": x * 2 + core}

    def index(stage, d):
        return sum((1 - v if b else v) * (1 << s) for s, (v, b) in enumerate(zip(labels[stage], _bits(d))))

    partner = {"outer": outer, "rows": pos[0] * 2 + 1 - core}
    everyone = [partner] + [peer(s, d) for s in range(2) for d in range(1, 8)]

    barrier = pltpu.get_barrier_semaphore()
    for dev in everyone:
        pl.semaphore_signal(barrier, inc=1, device_id=dev, device_id_type=MESH_T)
    pl.semaphore_wait(barrier, len(everyone))

    def copy(src, dst, send, recv, dev):
        return pltpu.make_async_remote_copy(src_ref=src, dst_ref=dst, send_sem=send, recv_sem=recv, device_id=dev, device_id_type=MESH_T)

    def piece(half, i):
        return pl.ds(pl.multiple_of(half * HALF + i * PIECE, PIECE), PIECE)

    sent = []

    def go(c):
        c.start()
        sent.append(c)
        return c

    first = [go(copy(p_ref.at[piece(1 - core, index(1, d))], rec0.at[d], s0.at[d], t0.at[d], partner)) for d in ORDER + (0,)]
    out1 = {}
    for n, d in enumerate(ORDER + (0,)):
        first[n].wait_recv()
        acc0[d] = p_ref[piece(core, index(0, d)), :] + rec0[d]
        if d:
            out1[d] = go(copy(acc0.at[d], rec1.at[d - 1], s1.at[d - 1], t1.at[d - 1], peer(0, d)))
    for d in range(1, 8):
        out1[d].wait_recv()
    total = acc0[0]
    for d in range(1, 8):
        total = total + rec1[d - 1]
    acc1[...] = total
    out2 = {}
    for e in ORDER:
        rows = pl.ds(pl.multiple_of(index(1, e) * CH, CH), CH)
        out2[e] = go(copy(acc1.at[rows], rec2.at[e - 1], s2.at[e - 1], t2.at[e - 1], peer(1, e)))
    for e in range(1, 8):
        out2[e].wait_recv()
    total = acc1[pl.ds(pl.multiple_of(index(1, 0) * CH, CH), CH), :]
    for e in range(1, 8):
        total = total + rec2[e - 1]

    def chunk(e):
        return pl.ds(pl.multiple_of(core * HALF + index(0, 0) * PIECE + index(1, e) * CH, CH), CH)

    o_ref[chunk(0), :] = total
    for e in ORDER:
        go(copy(o_ref.at[chunk(0)], o_ref.at[chunk(0)], s3.at[e - 1], t3.at[e - 1], peer(1, e)))
    for e in range(1, 8):
        copy(o_ref.at[chunk(e)], o_ref.at[chunk(e)], s3.at[e - 1], t3.at[e - 1], peer(1, e)).wait_recv()
    mine = piece(core, index(0, 0))
    for d in ORDER:
        go(copy(o_ref.at[mine], o_ref.at[mine], s4.at[d - 1], t4.at[d - 1], peer(0, d)))
    go(copy(o_ref.at[mine], o_ref.at[mine], s5.at[0], t5.at[0], partner))
    for d in (1, 2, 4, 3, 5, 6, 7):
        got = piece(core, index(0, d))
        copy(o_ref.at[got], o_ref.at[got], s4.at[d - 1], t4.at[d - 1], peer(0, d)).wait_recv()
        go(copy(o_ref.at[got], o_ref.at[got], s5.at[d], t5.at[d], partner))
    for d in range(8):
        got = piece(1 - core, index(1, d))
        copy(o_ref.at[got], o_ref.at[got], s5.at[d], t5.at[d], partner).wait_recv()
    for c in sent:
        c.wait_send()


def all_reduce(p, ident):
    sems = []
    for n in (8, 7, 7, 7, 7, 8):
        sems += [pltpu.SemaphoreType.DMA((n,))] * 2
    return pl.pallas_call(
        ar_kernel,
        out_shape=jax.ShapeDtypeStruct((ROWS_PACKED, B), jnp.float32),
        in_specs=[pl.BlockSpec(memory_space=pltpu.VMEM)],
        out_specs=pl.BlockSpec(memory_space=pltpu.VMEM),
        scratch_shapes=[
            pltpu.VMEM((8, PIECE, B), jnp.float32),
            pltpu.VMEM((8, PIECE, B), jnp.float32),
            pltpu.VMEM((7, PIECE, B), jnp.float32),
            pltpu.VMEM((PIECE, B), jnp.float32),
            pltpu.VMEM((7, CH, B), jnp.float32),
        ] + sems,
        compiler_params=pltpu.CompilerParams(collective_id=ident, has_side_effects=True),
        name="sum_group",
    )(p)


def solution(mesh):
    row_spec = P(("batch", "outer", "rows"), None)

    def local_qr(a):
        q1, p2, r1 = sweep_one(all_reduce(gram(a), 0), a)
        return tuple(sweep_two(all_reduce(p2, 1), q1, r1))

    return jax.shard_map(local_qr, mesh=mesh, in_specs=(row_spec,), out_specs=(row_spec, P("batch", None)), check_vma=False)
```

```python
import jax
import jax.numpy as jnp
from jax import lax
from jax.experimental import pallas as pl
from jax.experimental.pallas import tpu as pltpu
from jax.sharding import PartitionSpec as P

HI = lax.Precision.HIGHEST
N = 896
B = 128
NB = N // B
NG = B // 8


def dot(a, b, ca, cb):
    return lax.dot_general(a, b, (((ca,), (cb,)), ((), ())), precision=HI, preferred_element_type=jnp.float32)


def lane_col(v, c):
    lane = lax.broadcasted_iota(jnp.int32, (8, B), 1)
    return jnp.broadcast_to(jnp.sum(jnp.where(lane == c, v, 0.0), axis=1, keepdims=True), (8, B))


def sub_row(v, k):
    return jnp.broadcast_to(v[k:k + 1, :], (8, B))


def factor_diag(diag):
    sub = lax.broadcasted_iota(jnp.int32, (8, B), 0)
    lane = lax.broadcasted_iota(jnp.int32, (8, B), 1)
    m = list(diag)
    rows, inv = [None] * NG, [None] * NG
    for p in range(NG):
        g0 = 8 * p
        here = (lane >= g0) & (lane < g0 + 8)
        cols = [lane_col(m[p], g0 + k) for k in range(8)]
        z = jnp.where(here, jnp.where(lane == sub + g0, 1.0, 0.0), m[p])
        near = p + 1 < NG
        if near:
            cq = [lane_col(m[p + 1], g0 + k) for k in range(8)]
            mq = jnp.where(here, 0.0, m[p + 1])
        recs = jnp.zeros((8, B), jnp.float32)
        pivs = jnp.ones((8, B), jnp.float32)
        for k in range(8):
            piv = sub_row(cols[k], k)
            rec = 1.0 / piv
            pivs = jnp.where(sub == k, piv, pivs)
            recs = jnp.where(sub == k, rec, recs)
            low = jnp.where(sub > k, cols[k] * rec, 0.0)
            for kk in range(k + 1, 8):
                cross = sub_row(cols[kk], k)
                cols[kk] = cols[kk] - low * cross
                if near:
                    if kk == k + 1:
                        lq = cq[k] * rec
                    cq[kk] = cq[kk] - lq * cross
            if near and k == 7:
                lq = cq[k] * rec
            uz = sub_row(z, k)
            z = z - low * uz
            if near:
                mq = mq - lq * uz
        scale = lax.rsqrt(pivs)
        upper = z
        for kk in range(8):
            upper = jnp.where(lane == g0 + kk, cols[kk], upper)
        rows[p] = jnp.where(lane >= sub + g0, upper * scale, 0.0)
        inv[p] = jnp.where(lane < g0 + 8, z * scale, 0.0)
        if p + 2 < NG:
            wv = z * recs
            for kk in range(7, 0, -1):
                wv = wv - jnp.where(sub < kk, cols[kk] * recs, 0.0) * sub_row(wv, kk)
            wk = [sub_row(wv, k) for k in range(8)]
            for q in range(p + 2, NG):
                new = jnp.where(here, 0.0, m[q])
                for k in range(8):
                    new = new - lane_col(m[q], g0 + k) * wk[k]
                m[q] = new
        if near:
            m[p + 1] = mq
    return rows, inv


def block_row(i, j):
    return (i * NB - i * (i - 1) // 2 + j - i) * B


def mult(x):
    return pl.multiple_of(x, B)


def factor(g_ref, w, xd):
    w[:, N:] = jnp.zeros((N, N), jnp.float32)
    for i in range(NB):
        for j in range(i):
            w[i * B:(i + 1) * B, j * B:(j + 1) * B] = jnp.zeros((B, B), jnp.float32)
        for j in range(i, NB):
            w[i * B:(i + 1) * B, j * B:(j + 1) * B] = g_ref[pl.ds(block_row(i, j), B), :]

    def step(j, _):
        r0 = mult(j * B)
        rr = pl.ds(r0, B)
        group = [pl.ds(pl.multiple_of(r0 + 8 * q, 8), 8) for q in range(NG)]
        rows, inv = factor_diag([w[gq, pl.ds(r0, B)] for gq in group])
        for q in range(NG):
            w[group[q], pl.ds(r0, B)] = rows[q]
            w[group[q], pl.ds(mult(r0 + N), B)] = inv[q]
            xd[pl.ds(8 * q, 8), :] = inv[q]
        mid = pl.ds(mult(r0 + B), N - B)
        w[rr, mid] = dot(xd[...], w[rr, mid], 1, 0)
        odd = j % 2

        def trail(top, depth):
            src = pl.ds(mult(top), depth)
            win = pl.ds(mult(top + depth), N)

            def body(i, _):
                ri = pl.ds(mult(i * B), B)
                w[ri, win] = w[ri, win] - dot(w[src, ri], w[src, win], 0, 0)
                return 0

            return body

        lax.fori_loop(j + 1, jnp.where(odd == 0, jnp.minimum(j + 2, NB), j + 1), trail(r0, B), 0)
        lax.fori_loop(jnp.where(odd == 1, j + 1, NB), NB, trail(jnp.maximum(r0 - B, 0), 2 * B), 0)
        return 0

    lax.fori_loop(0, NB, step, 0)
    for i in range(1, NB):
        w[i * B:(i + 1) * B, :i * B] = jnp.zeros((B, i * B), jnp.float32)


M_LOC = 1024
STEP = 256
NSTEP = M_LOC // STEP
TILES = [(lo, min(lo + 256, N)) for lo in range(0, N, 256)]


def add_gram(rows, p_ref):
    for lo, hi in TILES:
        c = dot(rows[:, :hi], rows[:, lo:hi], 0, 0)
        for j in range(lo // B, hi // B):
            for i in range(j + 1):
                at = pl.ds(block_row(i, j), B)
                p_ref[at, :] = p_ref[at, :] + c[i * B:(i + 1) * B, j * B - lo:(j + 1) * B - lo]


def solve_rows(a, w, q):
    for lo, hi in TILES:
        q[:, lo:hi] = dot(a[:, :hi], w[lo:hi, N:N + hi], 1, 1)


def rows_at(s):
    return pl.ds(pl.multiple_of(s * STEP, STEP), STEP)


def gram_kernel(a_hbm, p_ref, a, sem):
    loads = [pltpu.make_async_copy(a_hbm.at[rows_at(s)], a.at[rows_at(s)], sem.at[s]) for s in range(NSTEP)]
    for c in loads:
        c.start()
    p_ref[...] = jnp.zeros(p_ref.shape, jnp.float32)

    def body(s, _):
        pltpu.make_async_copy(a_hbm.at[rows_at(s)], a.at[rows_at(s)], sem.at[s]).wait()
        add_gram(a.at[rows_at(s)], p_ref)
        return 0

    lax.fori_loop(0, NSTEP, body, 0)


def sweep_one_kernel(g_ref, a_hbm, q_hbm, p_ref, r_hbm, w, xd, a, q, sem, qsem):
    load = pltpu.make_async_copy(a_hbm, a, sem.at[0])
    load.start()
    p_ref[...] = jnp.zeros(p_ref.shape, jnp.float32)
    factor(g_ref, w, xd)
    keep = pltpu.make_async_copy(w.at[:, pl.ds(0, N)], r_hbm, sem.at[1])
    keep.start()
    load.wait()

    def body(s, _):
        at = rows_at(s)
        solve_rows(a.at[at], w, q.at[at])
        pltpu.make_async_copy(q.at[at], q_hbm.at[at], qsem.at[s]).start()
        add_gram(q.at[at], p_ref)
        return 0

    lax.fori_loop(0, NSTEP, body, 0)
    for s in range(NSTEP):
        pltpu.make_async_copy(q.at[rows_at(s)], q_hbm.at[rows_at(s)], qsem.at[s]).wait()
    keep.wait()


def sweep_two_kernel(g_ref, a_hbm, r1_hbm, q_hbm, r_hbm, w, xd, a, q, r1, r, sem, qsem, rsem):
    load = pltpu.make_async_copy(a_hbm, a, sem.at[0])
    load.start()
    load_r = pltpu.make_async_copy(r1_hbm, r1, sem.at[1])
    load_r.start()
    factor(g_ref, w, xd)
    load.wait()

    def body(s, _):
        at = rows_at(s)
        solve_rows(a.at[at], w, q.at[at])
        pltpu.make_async_copy(q.at[at], q_hbm.at[at], qsem.at[s]).start()
        return 0

    lax.fori_loop(0, NSTEP, body, 0)
    load_r.wait()
    stores = []
    for n, (lo, hi) in enumerate(TILES):
        if lo:
            r[lo:hi, :lo] = jnp.zeros((hi - lo, lo), jnp.float32)
        for clo, chi in TILES[n:]:
            r[lo:hi, clo:chi] = dot(w[lo:hi, lo:chi], r1[lo:chi, clo:chi], 1, 0)
        at = pl.ds(lo, hi - lo)
        stores.append(pltpu.make_async_copy(r.at[at], r_hbm.at[at], rsem.at[n]))
        stores[-1].start()
    for s in range(NSTEP):
        pltpu.make_async_copy(q.at[rows_at(s)], q_hbm.at[rows_at(s)], qsem.at[s]).wait()
    for c in stores:
        c.wait()


VM = pl.BlockSpec(memory_space=pltpu.VMEM)
ANY = pl.BlockSpec(memory_space=pl.ANY)
PARAMS = pltpu.CompilerParams(vmem_limit_bytes=58 * 2**20)
DMA = pltpu.SemaphoreType.DMA


def out(*s):
    return jax.ShapeDtypeStruct(s, jnp.float32)


def buf(*s):
    return pltpu.VMEM(s, jnp.float32)


def gram(a):
    return pl.pallas_call(
        gram_kernel, out_shape=out(ROWS_PACKED, B), in_specs=[ANY], out_specs=VM, name="gram",
        scratch_shapes=[buf(M_LOC, N), DMA((NSTEP,))], compiler_params=PARAMS,
    )(a)


def sweep_one(g, a):
    return pl.pallas_call(
        sweep_one_kernel, out_shape=[out(M_LOC, N), out(ROWS_PACKED, B), out(N, N)], in_specs=[VM, ANY], out_specs=[ANY, VM, ANY],
        scratch_shapes=[buf(N, 2 * N), buf(B, B), buf(M_LOC, N), buf(M_LOC, N), DMA((2,)), DMA((NSTEP,))],
        compiler_params=PARAMS, name="sweep_one",
    )(g, a)


def sweep_two(g, q1, r1):
    return pl.pallas_call(
        sweep_two_kernel, out_shape=[out(M_LOC, N), out(N, N)], in_specs=[VM, ANY, ANY], out_specs=[ANY, ANY],
        scratch_shapes=[buf(N, 2 * N), buf(B, B), buf(M_LOC, N), buf(M_LOC, N), buf(N, N), buf(N, N), DMA((2,)), DMA((NSTEP,)), DMA((4,))],
        compiler_params=PARAMS, name="sweep_two",
    )(g, q1, r1)


CH = 32
PAIR = 2 * CH
ROWS_PACKED = 128 * CH
SUMS = (2, 8, 4, PAIR, B)
MESH_T = pl.DeviceIdType.MESH
FAR_FIRST = (7, 3, 5, 6, 1, 2, 4)


def _bits(d):
    return tuple((d >> s) & 1 for s in range(3))


def _flip(v, kind):
    return (1 - kind) * (v + 1 - 2 * (v % 2)) + kind * (3 - v)


def _label(v, kind):
    return (1 - kind) * ((v % 2 + v // 2) % 2) + kind * (v // 2)


def ar_kernel(p_hbm, o_hbm, p, o, rec0, acc0, rec1, acc1, rec2, ld, st, s0, t0, s1, t1, s2, t2, s3, t3, s4, t4, s5, t5):
    outer, row = lax.axis_index("outer"), lax.axis_index("rows")
    pos = (row // 2, outer % 4, outer // 4)
    core = row % 2
    kinds = (core, 1 - core)
    labels = [tuple(_label(v, k) for v in pos) for k in kinds]

    def peer(stage, d):
        x, y, z = (_flip(v, kinds[stage]) if b else v for v, b in zip(pos, _bits(d)))
        return {"outer": z * 4 + y, "rows": x * 2 + core}

    def index(stage, d):
        return sum((1 - v if b else v) * (1 << s) for s, (v, b) in enumerate(zip(labels[stage], _bits(d))))

    def group(stage, g):
        return sum((1 - labels[stage][s] if (g >> (s - 1)) & 1 else labels[stage][s]) * (1 << (s - 1)) for s in (1, 2))

    def inside(e):
        v = labels[1][0]
        return pl.ds(pl.multiple_of((1 - v if e & 1 else v) * CH, CH), CH)

    partner = {"outer": outer, "rows": pos[0] * 2 + 1 - core}
    peers = [{d: peer(s, d) for d in range(1, 8)} for s in range(2)]
    idx = [index(0, d) for d in range(8)]
    grp = [[group(s, g) for g in range(4)] for s in range(2)]
    last_first = (3, 2, 1, 0)

    loads = [pltpu.make_async_copy(p_hbm.at[h], p.at[h], ld.at[n]) for n, h in enumerate((1 - core, core))]
    for c in loads:
        c.start()
    barrier = pltpu.get_barrier_semaphore()
    everyone = [partner, *peers[0].values(), *peers[1].values()]
    for dev in everyone:
        pl.semaphore_signal(barrier, inc=1, device_id=dev, device_id_type=MESH_T)
    loads[0].wait()
    pl.semaphore_wait(barrier, len(everyone))

    def copy(src, dst, send, recv, dev):
        return pltpu.make_async_remote_copy(src_ref=src, dst_ref=dst, send_sem=send, recv_sem=recv, device_id=dev, device_id_type=MESH_T)

    sent = []

    def go(c):
        c.start()
        sent.append(c)
        return c

    swap = {g: go(copy(p.at[1 - core, :, grp[0][g]], rec0.at[g], s0.at[g], t0.at[g], partner)) for g in last_first}
    loads[1].wait()
    out1 = {}
    for g in last_first:
        swap[g].wait_recv()
        acc0[g] = p[core, :, grp[1][g]] + rec0[g]
        for d in FAR_FIRST:
            out1[g, d] = go(copy(acc0.at[g, idx[d]], rec1.at[g, d - 1], s1.at[g, d - 1], t1.at[g, d - 1], peers[0][d]))
    out2 = {}
    for g in last_first:
        for d in range(1, 8):
            out1[g, d].wait_recv()
        total = acc0[g, idx[0]]
        for d in range(1, 8):
            total = total + rec1[g, d - 1]
        acc1[g] = total
        for e in (2 * g + 1, 2 * g):
            if e:
                out2[e] = go(copy(acc1.at[g, inside(e)], rec2.at[e - 1], s2.at[e - 1], t2.at[e - 1], peers[1][e]))
    for e in range(1, 8):
        out2[e].wait_recv()
    total = acc1[0, inside(0), :]
    for e in range(1, 8):
        total = total + rec2[e - 1]

    def chunk(e):
        return o.at[core, idx[0], grp[1][e // 2], inside(e)]

    o[core, idx[0], grp[1][0], inside(0), :] = total
    for e in FAR_FIRST:
        go(copy(chunk(0), chunk(0), s3.at[e - 1], t3.at[e - 1], peers[1][e]))
    for g in range(4):
        for e in (2 * g, 2 * g + 1):
            if e:
                copy(chunk(e), chunk(e), s3.at[e - 1], t3.at[e - 1], peers[1][e]).wait_recv()
        for d in FAR_FIRST:
            mine = o.at[core, idx[0], grp[1][g]]
            go(copy(mine, mine, s4.at[g, d - 1], t4.at[g, d - 1], peers[0][d]))
    stores = []

    def store(half, g, n):
        stores.append(pltpu.make_async_copy(o.at[half, :, g], o_hbm.at[half, :, g], st.at[n]))
        stores[-1].start()

    for g in range(4):
        for d in range(1, 8):
            got = o.at[core, idx[d], grp[1][g]]
            copy(got, got, s4.at[g, d - 1], t4.at[g, d - 1], peers[0][d]).wait_recv()
        whole = o.at[core, :, grp[1][g]]
        go(copy(whole, whole, s5.at[g], t5.at[g], partner))
        store(core, grp[1][g], g)
    for g in range(4):
        got = o.at[1 - core, :, grp[0][g]]
        copy(got, got, s5.at[g], t5.at[g], partner).wait_recv()
        store(1 - core, grp[0][g], 4 + g)
    for c in sent:
        c.wait_send()
    for c in stores:
        c.wait()


def all_reduce(p, ident):
    sems = [pltpu.SemaphoreType.DMA((2,)), pltpu.SemaphoreType.DMA((8,))]
    for n in ((4,), (4, 7), (7,), (7,), (4, 7), (4,)):
        sems += [pltpu.SemaphoreType.DMA(n)] * 2
    buf = lambda *s: pltpu.VMEM(s, jnp.float32)
    return pl.pallas_call(
        ar_kernel,
        out_shape=jax.ShapeDtypeStruct(SUMS, jnp.float32),
        in_specs=[pl.BlockSpec(memory_space=pl.ANY)],
        out_specs=pl.BlockSpec(memory_space=pl.ANY),
        scratch_shapes=[
            buf(*SUMS),
            buf(*SUMS),
            buf(4, 8, PAIR, B),
            buf(4, 8, PAIR, B),
            buf(4, 7, PAIR, B),
            buf(4, PAIR, B),
            buf(7, CH, B),
        ] + sems,
        compiler_params=pltpu.CompilerParams(collective_id=ident, has_side_effects=True, vmem_limit_bytes=40 * 2**20),
        name="sum_group",
    )(p.reshape(SUMS)).reshape(ROWS_PACKED, B)


def solution(mesh):
    row_spec = P(("batch", "outer", "rows"), None)

    def local_qr(a):
        q1, p2, r1 = sweep_one(all_reduce(gram(a), 0), a)
        return tuple(sweep_two(all_reduce(p2, 1), q1, r1))

    return jax.shard_map(local_qr, mesh=mesh, in_specs=(row_spec,), out_specs=(row_spec, P("batch", None)), check_vma=False)
```

```python
import jax
import jax.numpy as jnp
from jax import lax
from jax.experimental import pallas as pl
from jax.experimental.pallas import tpu as pltpu
from jax.sharding import PartitionSpec as P

HI = lax.Precision.HIGHEST
N = 896
B = 128
NB = N // B
NG = B // 8


def dot(a, b, ca, cb):
    return lax.dot_general(a, b, (((ca,), (cb,)), ((), ())), precision=HI, preferred_element_type=jnp.float32)


def lane_col(v, c):
    lane = lax.broadcasted_iota(jnp.int32, (8, B), 1)
    return jnp.broadcast_to(jnp.sum(jnp.where(lane == c, v, 0.0), axis=1, keepdims=True), (8, B))


def sub_row(v, k):
    return jnp.broadcast_to(v[k:k + 1, :], (8, B))


def factor_diag(diag):
    sub = lax.broadcasted_iota(jnp.int32, (8, B), 0)
    lane = lax.broadcasted_iota(jnp.int32, (8, B), 1)
    m = list(diag)
    rows, inv = [None] * NG, [None] * NG
    for p in range(NG // 2):
        g0 = 16 * p
        here = (lane >= g0) & (lane < g0 + 16)
        own = m[2 * p:2 * p + 2]
        cols = [[lane_col(own[r], g0 + k) for k in range(8 * r + 8)] for r in range(2)]
        dp = list(own)
        z = [jnp.where(here, jnp.where(lane == sub + (g0 + 8 * r), 1.0, 0.0), own[r]) for r in range(2)]
        near = m[2 * p + 2:2 * p + 4]
        cq = [[lane_col(v, g0 + k) for k in range(16)] for v in near]
        mq = [jnp.where(here, 0.0, v) for v in near]
        pivs = [jnp.ones((8, B), jnp.float32)] * 2
        for k in range(16):
            rk, sk = k // 8, k % 8
            piv = sub_row(cols[rk][k], sk)
            rec = 1.0 / piv
            pivs[rk] = jnp.where(sub == sk, piv, pivs[rk])
            for kk in range(k + 1, 16):
                t = sub_row(cols[kk // 8][k], kk % 8) * rec
                for r in range(kk // 8, 2):
                    cols[r][kk] = cols[r][kk] - cols[r][k] * t
                for c in cq:
                    c[kk] = c[kk] - c[k] * t
            v = sub_row(z[rk], sk) * rec
            y = sub_row(dp[rk], sk) * rec
            for r in range(rk, 2):
                low = jnp.where(sub > sk, cols[r][k], 0.0) if r == rk else cols[r][k]
                z[r] = z[r] - low * v
                dp[r] = dp[r] - low * y
            for n, c in enumerate(cq):
                mq[n] = mq[n] - c[k] * v
        scaled = []
        for r in range(2):
            scale = lax.rsqrt(pivs[r])
            scaled.append(z[r] * scale)
            rows[2 * p + r] = jnp.where(lane >= sub + (g0 + 8 * r), dp[r] * scale, 0.0)
            inv[2 * p + r] = jnp.where(lane < g0 + 16, scaled[r], 0.0)
        if 2 * p + 4 < NG:
            both = jnp.concatenate(scaled, axis=0)
            upd = dot(both, both, 0, 0)
            for q in range(2 * p + 4, NG):
                m[q] = jnp.where(here, 0.0, m[q]) - upd[8 * q:8 * q + 8, :]
        for n, v in enumerate(mq):
            m[2 * p + 2 + n] = v
    return rows, inv


def block_row(i, j):
    return (i * NB - i * (i - 1) // 2 + j - i) * B


def mult(x):
    return pl.multiple_of(x, B)


def factor(g_ref, w, xd):
    w[:, N:] = jnp.zeros((N, N), jnp.float32)
    for i in range(NB):
        for j in range(i):
            w[i * B:(i + 1) * B, j * B:(j + 1) * B] = jnp.zeros((B, B), jnp.float32)
        for j in range(i, NB):
            w[i * B:(i + 1) * B, j * B:(j + 1) * B] = g_ref[pl.ds(block_row(i, j), B), :]

    def step(j, _):
        r0 = mult(j * B)
        rr = pl.ds(r0, B)
        group = [pl.ds(pl.multiple_of(r0 + 8 * q, 8), 8) for q in range(NG)]
        rows, inv = factor_diag([w[gq, pl.ds(r0, B)] for gq in group])
        for q in range(NG):
            w[group[q], pl.ds(r0, B)] = rows[q]
            w[group[q], pl.ds(mult(r0 + N), B)] = inv[q]
            xd[pl.ds(8 * q, 8), :] = inv[q]
        mid = pl.ds(mult(r0 + B), N - B)
        w[rr, mid] = dot(xd[...], w[rr, mid], 1, 0)
        odd = j % 2

        def trail(top, depth):
            src = pl.ds(mult(top), depth)
            win = pl.ds(mult(top + depth), N)

            def body(i, _):
                ri = pl.ds(mult(i * B), B)
                w[ri, win] = w[ri, win] - dot(w[src, ri], w[src, win], 0, 0)
                return 0

            return body

        lax.fori_loop(j + 1, jnp.where(odd == 0, jnp.minimum(j + 2, NB), j + 1), trail(r0, B), 0)
        lax.fori_loop(jnp.where(odd == 1, j + 1, NB), NB, trail(jnp.maximum(r0 - B, 0), 2 * B), 0)
        return 0

    lax.fori_loop(0, NB, step, 0)
    for i in range(1, NB):
        w[i * B:(i + 1) * B, :i * B] = jnp.zeros((B, i * B), jnp.float32)


M_LOC = 1024
STEP = 256
NSTEP = M_LOC // STEP
TILES = [(lo, min(lo + 256, N)) for lo in range(0, N, 256)]


def add_gram(rows, p_ref):
    for lo, hi in TILES:
        c = dot(rows[:, :hi], rows[:, lo:hi], 0, 0)
        for j in range(lo // B, hi // B):
            for i in range(j + 1):
                at = pl.ds(block_row(i, j), B)
                p_ref[at, :] = p_ref[at, :] + c[i * B:(i + 1) * B, j * B - lo:(j + 1) * B - lo]


def solve_rows(a, w, q):
    for lo, hi in TILES:
        q[:, lo:hi] = dot(a[:, :hi], w[lo:hi, N:N + hi], 1, 1)


def rows_at(s):
    return pl.ds(pl.multiple_of(s * STEP, STEP), STEP)


def gram_kernel(a_hbm, p_ref, a, sem):
    loads = [pltpu.make_async_copy(a_hbm.at[rows_at(s)], a.at[rows_at(s)], sem.at[s]) for s in range(NSTEP)]
    for c in loads:
        c.start()
    p_ref[...] = jnp.zeros(p_ref.shape, jnp.float32)

    def body(s, _):
        pltpu.make_async_copy(a_hbm.at[rows_at(s)], a.at[rows_at(s)], sem.at[s]).wait()
        add_gram(a.at[rows_at(s)], p_ref)
        return 0

    lax.fori_loop(0, NSTEP, body, 0)


def sweep_one_kernel(g_ref, a_hbm, q_hbm, p_ref, r_hbm, w, xd, a, q, sem, qsem):
    load = pltpu.make_async_copy(a_hbm, a, sem.at[0])
    load.start()
    p_ref[...] = jnp.zeros(p_ref.shape, jnp.float32)
    factor(g_ref, w, xd)
    keep = pltpu.make_async_copy(w.at[:, pl.ds(0, N)], r_hbm, sem.at[1])
    keep.start()
    load.wait()

    def body(s, _):
        at = rows_at(s)
        solve_rows(a.at[at], w, q.at[at])
        pltpu.make_async_copy(q.at[at], q_hbm.at[at], qsem.at[s]).start()
        add_gram(q.at[at], p_ref)
        return 0

    lax.fori_loop(0, NSTEP, body, 0)
    for s in range(NSTEP):
        pltpu.make_async_copy(q.at[rows_at(s)], q_hbm.at[rows_at(s)], qsem.at[s]).wait()
    keep.wait()


def sweep_two_kernel(g_ref, a_hbm, r1_hbm, q_hbm, r_hbm, w, xd, a, q, r1, r, sem, qsem, rsem):
    load = pltpu.make_async_copy(a_hbm, a, sem.at[0])
    load.start()
    load_r = pltpu.make_async_copy(r1_hbm, r1, sem.at[1])
    load_r.start()
    factor(g_ref, w, xd)
    load.wait()

    def body(s, _):
        at = rows_at(s)
        solve_rows(a.at[at], w, q.at[at])
        pltpu.make_async_copy(q.at[at], q_hbm.at[at], qsem.at[s]).start()
        return 0

    lax.fori_loop(0, NSTEP, body, 0)
    load_r.wait()
    stores = []
    for n, (lo, hi) in enumerate(TILES):
        if lo:
            r[lo:hi, :lo] = jnp.zeros((hi - lo, lo), jnp.float32)
        for clo, chi in TILES[n:]:
            r[lo:hi, clo:chi] = dot(w[lo:hi, lo:chi], r1[lo:chi, clo:chi], 1, 0)
        at = pl.ds(lo, hi - lo)
        stores.append(pltpu.make_async_copy(r.at[at], r_hbm.at[at], rsem.at[n]))
        stores[-1].start()
    for s in range(NSTEP):
        pltpu.make_async_copy(q.at[rows_at(s)], q_hbm.at[rows_at(s)], qsem.at[s]).wait()
    for c in stores:
        c.wait()


VM = pl.BlockSpec(memory_space=pltpu.VMEM)
ANY = pl.BlockSpec(memory_space=pltpu.HBM)
PARAMS = pltpu.CompilerParams(vmem_limit_bytes=58 * 2**20)
DMA = pltpu.SemaphoreType.DMA


def out(*s):
    return jax.ShapeDtypeStruct(s, jnp.float32)


def buf(*s):
    return pltpu.VMEM(s, jnp.float32)


def gram(a):
    return pl.pallas_call(
        gram_kernel, out_shape=out(ROWS_PACKED, B), in_specs=[ANY], out_specs=VM, name="gram",
        scratch_shapes=[buf(M_LOC, N), DMA((NSTEP,))], compiler_params=PARAMS,
    )(a)


def sweep_one(g, a):
    return pl.pallas_call(
        sweep_one_kernel, out_shape=[out(M_LOC, N), out(ROWS_PACKED, B), out(N, N)], in_specs=[VM, ANY], out_specs=[ANY, VM, ANY],
        scratch_shapes=[buf(N, 2 * N), buf(B, B), buf(M_LOC, N), buf(M_LOC, N), DMA((2,)), DMA((NSTEP,))],
        compiler_params=PARAMS, name="sweep_one",
    )(g, a)


def sweep_two(g, q1, r1):
    return pl.pallas_call(
        sweep_two_kernel, out_shape=[out(M_LOC, N), out(N, N)], in_specs=[VM, ANY, ANY], out_specs=[ANY, ANY],
        scratch_shapes=[buf(N, 2 * N), buf(B, B), buf(M_LOC, N), buf(M_LOC, N), buf(N, N), buf(N, N), DMA((2,)), DMA((NSTEP,)), DMA((4,))],
        compiler_params=PARAMS, name="sweep_two",
    )(g, q1, r1)


CH = 32
PAIR = 2 * CH
ROWS_PACKED = 128 * CH
SUMS = (2, 8, 4, PAIR, B)
MESH_T = pl.DeviceIdType.MESH
FAR_FIRST = (7, 3, 5, 6, 1, 2, 4)


def _bits(d):
    return tuple((d >> s) & 1 for s in range(3))


def _flip(v, kind):
    return (1 - kind) * (v + 1 - 2 * (v % 2)) + kind * (3 - v)


def _label(v, kind):
    return (1 - kind) * ((v % 2 + v // 2) % 2) + kind * (v // 2)


def ar_kernel(p_hbm, o_hbm, p, o, rec0, acc0, rec1, acc1, rec2, ld, st, s0, t0, s1, t1, s2, t2, s3, t3, s4, t4, s5, t5):
    outer, row = lax.axis_index("outer"), lax.axis_index("rows")
    pos = (row // 2, outer % 4, outer // 4)
    core = row % 2
    kinds = (core, 1 - core)
    labels = [tuple(_label(v, k) for v in pos) for k in kinds]

    def peer(stage, d):
        x, y, z = (_flip(v, kinds[stage]) if b else v for v, b in zip(pos, _bits(d)))
        return {"outer": z * 4 + y, "rows": x * 2 + core}

    def index(stage, d):
        return sum((1 - v if b else v) * (1 << s) for s, (v, b) in enumerate(zip(labels[stage], _bits(d))))

    def group(stage, g):
        return sum((1 - labels[stage][s] if (g >> (s - 1)) & 1 else labels[stage][s]) * (1 << (s - 1)) for s in (1, 2))

    def inside(e):
        v = labels[1][0]
        return pl.ds(pl.multiple_of((1 - v if e & 1 else v) * CH, CH), CH)

    partner = {"outer": outer, "rows": pos[0] * 2 + 1 - core}
    peers = [{d: peer(s, d) for d in range(1, 8)} for s in range(2)]
    idx = [index(0, d) for d in range(8)]
    grp = [[group(s, g) for g in range(4)] for s in range(2)]
    last_first = (3, 2, 1, 0)

    loads = [pltpu.make_async_copy(p_hbm.at[h], p.at[h], ld.at[n]) for n, h in enumerate((1 - core, core))]
    for c in loads:
        c.start()
    barrier = pltpu.get_barrier_semaphore()
    everyone = [partner, *peers[0].values(), *peers[1].values()]
    for dev in everyone:
        pl.semaphore_signal(barrier, inc=1, device_id=dev, device_id_type=MESH_T)
    loads[0].wait()
    pl.semaphore_wait(barrier, len(everyone))

    def copy(src, dst, send, recv, dev):
        return pltpu.make_async_remote_copy(src_ref=src, dst_ref=dst, send_sem=send, recv_sem=recv, device_id=dev, device_id_type=MESH_T)

    sent = []

    def go(c):
        c.start()
        sent.append(c)
        return c

    swap = {g: go(copy(p.at[1 - core, :, grp[0][g]], rec0.at[g], s0.at[g], t0.at[g], partner)) for g in last_first}
    loads[1].wait()
    out1 = {}
    for g in last_first:
        swap[g].wait_recv()
        acc0[g] = p[core, :, grp[1][g]] + rec0[g]
        for d in FAR_FIRST:
            out1[g, d] = go(copy(acc0.at[g, idx[d]], rec1.at[g, d - 1], s1.at[g, d - 1], t1.at[g, d - 1], peers[0][d]))
    out2 = {}
    for g in last_first:
        for d in range(1, 8):
            out1[g, d].wait_recv()
        total = acc0[g, idx[0]]
        for d in range(1, 8):
            total = total + rec1[g, d - 1]
        acc1[g] = total
        for e in (2 * g + 1, 2 * g):
            if e:
                out2[e] = go(copy(acc1.at[g, inside(e)], rec2.at[e - 1], s2.at[e - 1], t2.at[e - 1], peers[1][e]))
    for e in range(1, 8):
        out2[e].wait_recv()
    total = acc1[0, inside(0), :]
    for e in range(1, 8):
        total = total + rec2[e - 1]

    def chunk(e):
        return o.at[core, idx[0], grp[1][e // 2], inside(e)]

    o[core, idx[0], grp[1][0], inside(0), :] = total
    for e in FAR_FIRST:
        go(copy(chunk(0), chunk(0), s3.at[e - 1], t3.at[e - 1], peers[1][e]))
    for g in range(4):
        for e in (2 * g, 2 * g + 1):
            if e:
                copy(chunk(e), chunk(e), s3.at[e - 1], t3.at[e - 1], peers[1][e]).wait_recv()
        for d in FAR_FIRST:
            mine = o.at[core, idx[0], grp[1][g]]
            go(copy(mine, mine, s4.at[g, d - 1], t4.at[g, d - 1], peers[0][d]))
    stores = []

    def store(half, g, n):
        stores.append(pltpu.make_async_copy(o.at[half, :, g], o_hbm.at[half, :, g], st.at[n]))
        stores[-1].start()

    for g in range(4):
        for d in range(1, 8):
            got = o.at[core, idx[d], grp[1][g]]
            copy(got, got, s4.at[g, d - 1], t4.at[g, d - 1], peers[0][d]).wait_recv()
        whole = o.at[core, :, grp[1][g]]
        go(copy(whole, whole, s5.at[g], t5.at[g], partner))
        store(core, grp[1][g], g)
    for g in range(4):
        got = o.at[1 - core, :, grp[0][g]]
        copy(got, got, s5.at[g], t5.at[g], partner).wait_recv()
        store(1 - core, grp[0][g], 4 + g)
    for c in sent:
        c.wait_send()
    for c in stores:
        c.wait()


def all_reduce(p, ident):
    sems = [pltpu.SemaphoreType.DMA((2,)), pltpu.SemaphoreType.DMA((8,))]
    for n in ((4,), (4, 7), (7,), (7,), (4, 7), (4,)):
        sems += [pltpu.SemaphoreType.DMA(n)] * 2
    buf = lambda *s: pltpu.VMEM(s, jnp.float32)
    return pl.pallas_call(
        ar_kernel,
        out_shape=jax.ShapeDtypeStruct(SUMS, jnp.float32),
        in_specs=[pl.BlockSpec(memory_space=pltpu.HBM)],
        out_specs=pl.BlockSpec(memory_space=pltpu.HBM),
        scratch_shapes=[
            buf(*SUMS),
            buf(*SUMS),
            buf(4, 8, PAIR, B),
            buf(4, 8, PAIR, B),
            buf(4, 7, PAIR, B),
            buf(4, PAIR, B),
            buf(7, CH, B),
        ] + sems,
        compiler_params=pltpu.CompilerParams(collective_id=ident, has_side_effects=True, vmem_limit_bytes=63 * 2**20),
        name="sum_group",
    )(p.reshape(SUMS)).reshape(ROWS_PACKED, B)


def solution(mesh):
    row_spec = P(("batch", "outer", "rows"), None)

    def local_qr(a):
        q1, p2, r1 = sweep_one(all_reduce(gram(a), 0), a)
        return tuple(sweep_two(all_reduce(p2, 1), q1, r1))

    return jax.shard_map(local_qr, mesh=mesh, in_specs=(row_spec,), out_specs=(row_spec, P("batch", None)), check_vma=False)
```

```python
import jax
import jax.numpy as jnp
from jax import lax
from jax.experimental import pallas as pl
from jax.experimental.pallas import tpu as pltpu
from jax.sharding import PartitionSpec as P

HI = lax.Precision.HIGHEST
N = 896
B = 128
NB = N // B
NG = B // 8


def dot(a, b, ca, cb):
    return lax.dot_general(a, b, (((ca,), (cb,)), ((), ())), precision=HI, preferred_element_type=jnp.float32)


def lane_col(v, c):
    lane = lax.broadcasted_iota(jnp.int32, (8, B), 1)
    return jnp.broadcast_to(jnp.sum(jnp.where(lane == c, v, 0.0), axis=1, keepdims=True), (8, B))


def sub_row(v, k):
    return jnp.broadcast_to(v[k:k + 1, :], (8, B))


def factor_diag(diag):
    sub = lax.broadcasted_iota(jnp.int32, (8, B), 0)
    lane = lax.broadcasted_iota(jnp.int32, (8, B), 1)
    m = list(diag)
    rows, inv = [None] * NG, [None] * NG
    for p in range(NG // 2):
        g0 = 16 * p
        here = (lane >= g0) & (lane < g0 + 16)
        own = m[2 * p:2 * p + 2]
        cols = [[lane_col(own[r], g0 + k) for k in range(8 * r + 8)] for r in range(2)]
        dp = list(own)
        z = [jnp.where(here, jnp.where(lane == sub + (g0 + 8 * r), 1.0, 0.0), own[r]) for r in range(2)]
        near = m[2 * p + 2:2 * p + 4]
        cq = [[lane_col(v, g0 + k) for k in range(16)] for v in near]
        mq = [jnp.where(here, 0.0, v) for v in near]
        pivs = [jnp.ones((8, B), jnp.float32)] * 2
        for k in range(16):
            rk, sk = k // 8, k % 8
            piv = sub_row(cols[rk][k], sk)
            rec = 1.0 / piv
            pivs[rk] = jnp.where(sub == sk, piv, pivs[rk])
            for kk in range(k + 1, 16):
                t = sub_row(cols[kk // 8][k], kk % 8) * rec
                for r in range(kk // 8, 2):
                    cols[r][kk] = cols[r][kk] - cols[r][k] * t
                for c in cq:
                    c[kk] = c[kk] - c[k] * t
            v = sub_row(z[rk], sk) * rec
            y = sub_row(dp[rk], sk) * rec
            for r in range(rk, 2):
                low = jnp.where(sub > sk, cols[r][k], 0.0) if r == rk else cols[r][k]
                z[r] = z[r] - low * v
                dp[r] = dp[r] - low * y
            for n, c in enumerate(cq):
                mq[n] = mq[n] - c[k] * v
        scaled = []
        for r in range(2):
            scale = lax.rsqrt(pivs[r])
            scaled.append(z[r] * scale)
            rows[2 * p + r] = jnp.where(lane >= sub + (g0 + 8 * r), dp[r] * scale, 0.0)
            inv[2 * p + r] = jnp.where(lane < g0 + 16, scaled[r], 0.0)
        if 2 * p + 4 < NG:
            both = jnp.concatenate(scaled, axis=0)
            upd = dot(both, both, 0, 0)
            for q in range(2 * p + 4, NG):
                m[q] = jnp.where(here, 0.0, m[q]) - upd[8 * q:8 * q + 8, :]
        for n, v in enumerate(mq):
            m[2 * p + 2 + n] = v
    return rows, inv


TILES = [(lo, min(lo + 256, N)) for lo in range(0, N, 256)]
TILE_ORDER = (3, 1, 2, 0)
CH = 32
PAIR = 2 * CH
SUMS = (2, 8, 4, PAIR, B)


def _places():
    blocks = [(i, j) for t in TILE_ORDER for j in range(TILES[t][0] // B, TILES[t][1] // B) for i in range(j + 1)]
    return {b: (n % 7 // 4, n % 7 % 4 * 2, n // 7) for n, b in enumerate(blocks)}


PLACE = _places()


def read_block(g_ref, i, j):
    h, m, quarter = PLACE[i, j]
    return g_ref[h, m:m + 2, quarter].reshape(B, B)


def mult(x):
    return pl.multiple_of(x, B)


def factor(g_ref, w, xd):
    w[:, N:] = jnp.zeros((N, N), jnp.float32)
    for i in range(NB):
        for j in range(i):
            w[i * B:(i + 1) * B, j * B:(j + 1) * B] = jnp.zeros((B, B), jnp.float32)
        for j in range(i, NB):
            w[i * B:(i + 1) * B, j * B:(j + 1) * B] = read_block(g_ref, i, j)

    def step(j, _):
        r0 = mult(j * B)
        rr = pl.ds(r0, B)
        group = [pl.ds(pl.multiple_of(r0 + 8 * q, 8), 8) for q in range(NG)]
        rows, inv = factor_diag([w[gq, pl.ds(r0, B)] for gq in group])
        for q in range(NG):
            w[group[q], pl.ds(r0, B)] = rows[q]
            w[group[q], pl.ds(mult(r0 + N), B)] = inv[q]
            xd[pl.ds(8 * q, 8), :] = inv[q]
        mid = pl.ds(mult(r0 + B), N - B)
        w[rr, mid] = dot(xd[...], w[rr, mid], 1, 0)
        odd = j % 2

        def trail(top, depth):
            src = pl.ds(mult(top), depth)
            win = pl.ds(mult(top + depth), N)

            def body(i, _):
                ri = pl.ds(mult(i * B), B)
                w[ri, win] = w[ri, win] - dot(w[src, ri], w[src, win], 0, 0)
                return 0

            return body

        lax.fori_loop(j + 1, jnp.where(odd == 0, jnp.minimum(j + 2, NB), j + 1), trail(r0, B), 0)
        lax.fori_loop(jnp.where(odd == 1, j + 1, NB), NB, trail(jnp.maximum(r0 - B, 0), 2 * B), 0)
        return 0

    lax.fori_loop(0, NB, step, 0)
    for i in range(1, NB):
        w[i * B:(i + 1) * B, :i * B] = jnp.zeros((B, i * B), jnp.float32)


M_LOC = 1024
STEP = 256
NSTEP = M_LOC // STEP


def solve_rows(a, w, q):
    for lo, hi in TILES:
        q[:, lo:hi] = dot(a[:, :hi], w[lo:hi, N:N + hi], 1, 1)


def rows_at(s):
    return pl.ds(pl.multiple_of(s * STEP, STEP), STEP)


MESH_T = pl.DeviceIdType.MESH
FAR_FIRST = (7, 3, 5, 6, 1, 2, 4)


def _bits(d):
    return tuple((d >> s) & 1 for s in range(3))


def _flip(v, kind):
    return (1 - kind) * (v + 1 - 2 * (v % 2)) + kind * (3 - v)


def _label(v, kind):
    return (1 - kind) * ((v % 2 + v // 2) % 2) + kind * (v // 2)


class Net:
    def __init__(self):
        outer, row = lax.axis_index("outer"), lax.axis_index("rows")
        pos = (row // 2, outer % 4, outer // 4)
        self.core = core = row % 2
        kinds = (core, 1 - core)
        labels = [tuple(_label(v, k) for v in pos) for k in kinds]
        self.low = labels[1][0]

        def peer(stage, d):
            x, y, z = (_flip(v, kinds[stage]) if b else v for v, b in zip(pos, _bits(d)))
            return {"outer": z * 4 + y, "rows": x * 2 + core}

        def group(stage, g):
            return sum((1 - labels[stage][s] if (g >> (s - 1)) & 1 else labels[stage][s]) * (1 << (s - 1)) for s in (1, 2))

        self.partner = {"outer": outer, "rows": pos[0] * 2 + 1 - core}
        self.peers = [{d: peer(s, d) for d in range(1, 8)} for s in range(2)]
        self.idx = [sum((1 - v if b else v) * (1 << s) for s, (v, b) in enumerate(zip(labels[0], _bits(d)))) for d in range(8)]
        self.grp = [[group(s, g) for g in range(4)] for s in range(2)]
        self.everyone = [self.partner, *self.peers[0].values(), *self.peers[1].values()]

    def inside(self, e):
        return pl.ds(pl.multiple_of((1 - self.low if e & 1 else self.low) * CH, CH), CH)

    def announce(self):
        for dev in self.everyone:
            pl.semaphore_signal(pltpu.get_barrier_semaphore(), inc=1, device_id=dev, device_id_type=MESH_T)

    def meet(self):
        pl.semaphore_wait(pltpu.get_barrier_semaphore(), len(self.everyone))


def gram_sum(net, a, ready, o_hbm, p, o, rec0, acc0, rec1, acc1, rec2, st, s0, t0, s1, t1, s2, t2, s3, t3, s4, t4, s5, t5):
    core, partner, peers, idx, grp = net.core, net.partner, net.peers, net.idx, net.grp

    def copy(src, dst, send, recv, dev):
        return pltpu.make_async_remote_copy(src_ref=src, dst_ref=dst, send_sem=send, recv_sem=recv, device_id=dev, device_id_type=MESH_T)

    sent = []

    def go(c):
        c.start()
        sent.append(c)
        return c

    def tile(t, wait):
        lo, hi = TILES[t]

        def body(s, _):
            if wait:
                ready(s)
            at = rows_at(s)
            c = dot(a[at, :hi], a[at, lo:hi], 0, 0)
            for j in range(lo // B, hi // B):
                for i in range(j + 1):
                    h, m, quarter = PLACE[i, j]
                    c_ij = c[i * B:(i + 1) * B, j * B - lo:(j + 1) * B - lo]
                    p[h, m:m + 2, quarter] = p[h, m:m + 2, quarter] + c_ij.reshape(2, PAIR, B)
            return 0

        lax.fori_loop(0, NSTEP, body, 0)

    swap = {}

    def exchange(quarter):
        swap[quarter] = go(copy(p.at[1 - core, :, quarter], rec0.at[quarter], s0.at[quarter], t0.at[quarter], partner))

    def out1(quarter, d):
        return copy(acc0.at[quarter, idx[d]], rec1.at[quarter, d - 1], s1.at[quarter, d - 1], t1.at[quarter, d - 1], peers[0][d])

    def scatter(quarter):
        swap[quarter].wait_recv()
        acc0[quarter] = p[core, :, quarter] + rec0[quarter]
        for d in FAR_FIRST:
            go(out1(quarter, d))

    tile(TILE_ORDER[0], True)
    net.meet()
    exchange(0)
    for quarter in range(1, 4):
        tile(TILE_ORDER[quarter], False)
        exchange(quarter)
        scatter(quarter - 1)
    scatter(3)
    out2 = {}
    for g in (3, 2, 1, 0):
        quarter = grp[1][g]
        for d in range(1, 8):
            out1(quarter, d).wait_recv()
        total = acc0[quarter, idx[0]]
        for d in range(1, 8):
            total = total + rec1[quarter, d - 1]
        acc1[g] = total
        for e in (2 * g + 1, 2 * g):
            if e:
                out2[e] = go(copy(acc1.at[g, net.inside(e)], rec2.at[e - 1], s2.at[e - 1], t2.at[e - 1], peers[1][e]))
    for e in range(1, 8):
        out2[e].wait_recv()
    total = acc1[0, net.inside(0), :]
    for e in range(1, 8):
        total = total + rec2[e - 1]

    def chunk(e):
        return o.at[core, idx[0], grp[1][e // 2], net.inside(e)]

    o[core, idx[0], grp[1][0], net.inside(0), :] = total
    for e in FAR_FIRST:
        go(copy(chunk(0), chunk(0), s3.at[e - 1], t3.at[e - 1], peers[1][e]))
    for g in range(4):
        for e in (2 * g, 2 * g + 1):
            if e:
                copy(chunk(e), chunk(e), s3.at[e - 1], t3.at[e - 1], peers[1][e]).wait_recv()
        for d in FAR_FIRST:
            mine = o.at[core, idx[0], grp[1][g]]
            go(copy(mine, mine, s4.at[g, d - 1], t4.at[g, d - 1], peers[0][d]))
    stores = []

    def store(half, g, n):
        stores.append(pltpu.make_async_copy(o.at[half, :, g], o_hbm.at[half, :, g], st.at[n]))
        stores[-1].start()

    for g in range(4):
        for d in range(1, 8):
            got = o.at[core, idx[d], grp[1][g]]
            copy(got, got, s4.at[g, d - 1], t4.at[g, d - 1], peers[0][d]).wait_recv()
        whole = o.at[core, :, grp[1][g]]
        go(copy(whole, whole, s5.at[g], t5.at[g], partner))
        store(core, grp[1][g], g)
    for g in range(4):
        got = o.at[1 - core, :, grp[0][g]]
        copy(got, got, s5.at[g], t5.at[g], partner).wait_recv()
        store(1 - core, grp[0][g], 4 + g)
    for c in sent:
        c.wait_send()
    for c in stores:
        c.wait()


def gram_kernel(a_hbm, o_hbm, a, sem, p, *rest):
    net = Net()
    net.announce()

    def part(s):
        return pltpu.make_async_copy(a_hbm.at[rows_at(s)], a.at[rows_at(s)], sem.at[s])

    for s in range(NSTEP):
        part(s).start()
    p[...] = jnp.zeros(SUMS, jnp.float32)
    gram_sum(net, a, lambda s: part(s).wait(), o_hbm, p, *rest)


def sweep_one_kernel(g_ref, a_hbm, q_hbm, o_hbm, r_hbm, w, xd, a, q, sem, qsem, p, *rest):
    net = Net()
    net.announce()
    load = pltpu.make_async_copy(a_hbm, a, sem.at[0])
    load.start()
    p[...] = jnp.zeros(SUMS, jnp.float32)
    factor(g_ref, w, xd)
    keep = pltpu.make_async_copy(w.at[:, pl.ds(0, N)], r_hbm, sem.at[1])
    keep.start()
    load.wait()

    def part(s):
        return pltpu.make_async_copy(q.at[rows_at(s)], q_hbm.at[rows_at(s)], qsem.at[s])

    def body(s, _):
        solve_rows(a.at[rows_at(s)], w, q.at[rows_at(s)])
        part(s).start()
        return 0

    lax.fori_loop(0, NSTEP, body, 0)
    gram_sum(net, q, lambda s: None, o_hbm, p, *rest)
    for s in range(NSTEP):
        part(s).wait()
    keep.wait()


def sweep_two_kernel(g_ref, a_hbm, r1_hbm, q_hbm, r_hbm, w, xd, a, q, r1, r, sem, qsem, rsem):
    load = pltpu.make_async_copy(a_hbm, a, sem.at[0])
    load.start()
    load_r = pltpu.make_async_copy(r1_hbm, r1, sem.at[1])
    load_r.start()
    factor(g_ref, w, xd)
    load.wait()

    def body(s, _):
        at = rows_at(s)
        solve_rows(a.at[at], w, q.at[at])
        pltpu.make_async_copy(q.at[at], q_hbm.at[at], qsem.at[s]).start()
        return 0

    lax.fori_loop(0, NSTEP, body, 0)
    load_r.wait()
    stores = []
    for n, (lo, hi) in enumerate(TILES):
        if lo:
            r[lo:hi, :lo] = jnp.zeros((hi - lo, lo), jnp.float32)
        for clo, chi in TILES[n:]:
            r[lo:hi, clo:chi] = dot(w[lo:hi, lo:chi], r1[lo:chi, clo:chi], 1, 0)
        at = pl.ds(lo, hi - lo)
        stores.append(pltpu.make_async_copy(r.at[at], r_hbm.at[at], rsem.at[n]))
        stores[-1].start()
    for s in range(NSTEP):
        pltpu.make_async_copy(q.at[rows_at(s)], q_hbm.at[rows_at(s)], qsem.at[s]).wait()
    for c in stores:
        c.wait()


VM = pl.BlockSpec(memory_space=pltpu.VMEM)
ANY = pl.BlockSpec(memory_space=pltpu.HBM)
PARAMS = pltpu.CompilerParams(vmem_limit_bytes=63 * 2**20)
DMA = pltpu.SemaphoreType.DMA


def out(*s):
    return jax.ShapeDtypeStruct(s, jnp.float32)


def buf(*s):
    return pltpu.VMEM(s, jnp.float32)


def sum_scratch():
    sems = [DMA((8,))]
    for n in ((4,), (4, 7), (7,), (7,), (4, 7), (4,)):
        sems += [DMA(n)] * 2
    return [buf(*SUMS), buf(*SUMS), buf(4, 8, PAIR, B), buf(4, 8, PAIR, B), buf(4, 7, PAIR, B), buf(4, PAIR, B), buf(7, CH, B)] + sems


def remote(ident):
    return pltpu.CompilerParams(collective_id=ident, has_side_effects=True, vmem_limit_bytes=63 * 2**20)


def gram(a):
    return pl.pallas_call(
        gram_kernel, out_shape=out(*SUMS), in_specs=[ANY], out_specs=ANY, name="gram",
        scratch_shapes=[buf(M_LOC, N), DMA((NSTEP,))] + sum_scratch(), compiler_params=remote(0),
    )(a)


def sweep_one(g, a):
    return pl.pallas_call(
        sweep_one_kernel, out_shape=[out(M_LOC, N), out(*SUMS), out(N, N)], in_specs=[VM, ANY], out_specs=[ANY, ANY, ANY],
        scratch_shapes=[buf(N, 2 * N), buf(B, B), buf(M_LOC, N), buf(M_LOC, N), DMA((2,)), DMA((NSTEP,))] + sum_scratch(),
        compiler_params=remote(1), name="sweep_one",
    )(g, a)


def sweep_two(g, q1, r1):
    return pl.pallas_call(
        sweep_two_kernel, out_shape=[out(M_LOC, N), out(N, N)], in_specs=[VM, ANY, ANY], out_specs=[ANY, ANY],
        scratch_shapes=[buf(N, 2 * N), buf(B, B), buf(M_LOC, N), buf(M_LOC, N), buf(N, N), buf(N, N), DMA((2,)), DMA((NSTEP,)), DMA((4,))],
        compiler_params=PARAMS, name="sweep_two",
    )(g, q1, r1)


def solution(mesh):
    row_spec = P(("batch", "outer", "rows"), None)

    def local_qr(a):
        q1, g2, r1 = sweep_one(gram(a), a)
        return tuple(sweep_two(g2, q1, r1))

    return jax.shard_map(local_qr, mesh=mesh, in_specs=(row_spec,), out_specs=(row_spec, P("batch", None)), check_vma=False)
```

```python
import jax
import jax.numpy as jnp
from jax import lax
from jax.experimental import pallas as pl
from jax.experimental.pallas import tpu as pltpu
from jax.sharding import PartitionSpec as P

HI = lax.Precision.HIGHEST
N = 896
B = 128
NB = N // B
NG = B // 8


def dot(a, b, ca, cb):
    return lax.dot_general(a, b, (((ca,), (cb,)), ((), ())), precision=HI, preferred_element_type=jnp.float32)


def lane_col(v, c):
    lane = lax.broadcasted_iota(jnp.int32, (8, B), 1)
    return jnp.broadcast_to(jnp.sum(jnp.where(lane == c, v, 0.0), axis=1, keepdims=True), (8, B))


def sub_row(v, k):
    return jnp.broadcast_to(v[k:k + 1, :], (8, B))


def factor_diag(diag):
    sub = lax.broadcasted_iota(jnp.int32, (8, B), 0)
    lane = lax.broadcasted_iota(jnp.int32, (8, B), 1)
    m = list(diag)
    rows, inv = [None] * NG, [None] * NG
    for p in range(NG // 2):
        g0 = 16 * p
        here = (lane >= g0) & (lane < g0 + 16)
        own = m[2 * p:2 * p + 2]
        cols = [[lane_col(own[r], g0 + k) for k in range(8 * r + 8)] for r in range(2)]
        dp = list(own)
        z = [jnp.where(here, jnp.where(lane == sub + (g0 + 8 * r), 1.0, 0.0), own[r]) for r in range(2)]
        near = m[2 * p + 2:2 * p + 4]
        cq = [[lane_col(v, g0 + k) for k in range(16)] for v in near]
        mq = [jnp.where(here, 0.0, v) for v in near]
        pivs = [jnp.ones((8, B), jnp.float32)] * 2
        for k in range(16):
            rk, sk = k // 8, k % 8
            piv = sub_row(cols[rk][k], sk)
            rec = 1.0 / piv
            pivs[rk] = jnp.where(sub == sk, piv, pivs[rk])
            for kk in range(k + 1, 16):
                t = sub_row(cols[kk // 8][k], kk % 8) * rec
                for r in range(kk // 8, 2):
                    cols[r][kk] = cols[r][kk] - cols[r][k] * t
                for c in cq:
                    c[kk] = c[kk] - c[k] * t
            v = sub_row(z[rk], sk) * rec
            y = sub_row(dp[rk], sk) * rec
            for r in range(rk, 2):
                low = jnp.where(sub > sk, cols[r][k], 0.0) if r == rk else cols[r][k]
                z[r] = z[r] - low * v
                dp[r] = dp[r] - low * y
            for n, c in enumerate(cq):
                mq[n] = mq[n] - c[k] * v
        scaled = []
        for r in range(2):
            scale = lax.rsqrt(pivs[r])
            scaled.append(z[r] * scale)
            rows[2 * p + r] = jnp.where(lane >= sub + (g0 + 8 * r), dp[r] * scale, 0.0)
            inv[2 * p + r] = jnp.where(lane < g0 + 16, scaled[r], 0.0)
        if 2 * p + 4 < NG:
            both = jnp.concatenate(scaled, axis=0)
            upd = dot(both, both, 0, 0)
            for q in range(2 * p + 4, NG):
                m[q] = jnp.where(here, 0.0, m[q]) - upd[8 * q:8 * q + 8, :]
        for n, v in enumerate(mq):
            m[2 * p + 2 + n] = v
    return rows, inv


TILES = [(lo, min(lo + 256, N)) for lo in range(0, N, 256)]
TILE_ORDER = (3, 1, 2, 0)
CH = 32
PAIR = 2 * CH
SUMS = (2, 8, 4, PAIR, B)


def _places():
    blocks = [(i, j) for t in TILE_ORDER for j in range(TILES[t][0] // B, TILES[t][1] // B) for i in range(j + 1)]
    return {b: (n % 7 // 4, n % 7 % 4 * 2, n // 7) for n, b in enumerate(blocks)}


PLACE = _places()


def read_block(g_ref, i, j):
    h, m, quarter = PLACE[i, j]
    return g_ref[h, m:m + 2, quarter].reshape(B, B)


def mult(x):
    return pl.multiple_of(x, B)


def clear(w):
    w[:, N:] = jnp.zeros((N, N), jnp.float32)
    for i in range(1, NB):
        w[i * B:(i + 1) * B, :i * B] = jnp.zeros((B, i * B), jnp.float32)


def factor(g_ref, w, xd):
    for i in range(NB):
        for j in range(i, NB):
            w[i * B:(i + 1) * B, j * B:(j + 1) * B] = read_block(g_ref, i, j)

    def step(j, _):
        r0 = mult(j * B)
        rr = pl.ds(r0, B)
        group = [pl.ds(pl.multiple_of(r0 + 8 * q, 8), 8) for q in range(NG)]
        rows, inv = factor_diag([w[gq, pl.ds(r0, B)] for gq in group])
        for q in range(NG):
            w[group[q], pl.ds(r0, B)] = rows[q]
            w[group[q], pl.ds(mult(r0 + N), B)] = inv[q]
            xd[pl.ds(8 * q, 8), :] = inv[q]
        mid = pl.ds(mult(r0 + B), N - B)
        w[rr, mid] = dot(xd[...], w[rr, mid], 1, 0)
        odd = j % 2

        def trail(top, depth):
            src = pl.ds(mult(top), depth)
            win = pl.ds(mult(top + depth), N)

            def body(i, _):
                ri = pl.ds(mult(i * B), B)
                w[ri, win] = w[ri, win] - dot(w[src, ri], w[src, win], 0, 0)
                return 0

            return body

        lax.fori_loop(j + 1, jnp.where(odd == 0, jnp.minimum(j + 2, NB), j + 1), trail(r0, B), 0)
        lax.fori_loop(jnp.where(odd == 1, j + 1, NB), NB, trail(jnp.maximum(r0 - B, 0), 2 * B), 0)
        return 0

    lax.fori_loop(0, NB, step, 0)
    for i in range(1, NB):
        w[i * B:(i + 1) * B, :i * B] = jnp.zeros((B, i * B), jnp.float32)


M_LOC = 1024
STEP = 256
NSTEP = M_LOC // STEP


def solve_rows(a, w, q):
    for lo, hi in TILES:
        q[:, lo:hi] = dot(a[:, :hi], w[lo:hi, N:N + hi], 1, 1)


def rows_at(s):
    return pl.ds(pl.multiple_of(s * STEP, STEP), STEP)


MESH_T = pl.DeviceIdType.MESH
FAR_FIRST = (7, 3, 5, 6, 1, 2, 4)


def _bits(d):
    return tuple((d >> s) & 1 for s in range(3))


def _flip(v, kind):
    return (1 - kind) * (v + 1 - 2 * (v % 2)) + kind * (3 - v)


def _label(v, kind):
    return (1 - kind) * ((v % 2 + v // 2) % 2) + kind * (v // 2)


class Net:
    def __init__(self):
        outer, row = lax.axis_index("outer"), lax.axis_index("rows")
        pos = (row // 2, outer % 4, outer // 4)
        self.core = core = row % 2
        kinds = (core, 1 - core)
        labels = [tuple(_label(v, k) for v in pos) for k in kinds]
        self.low = labels[1][0]

        def peer(stage, d):
            x, y, z = (_flip(v, kinds[stage]) if b else v for v, b in zip(pos, _bits(d)))
            return {"outer": z * 4 + y, "rows": x * 2 + core}

        def group(stage, g):
            return sum((1 - labels[stage][s] if (g >> (s - 1)) & 1 else labels[stage][s]) * (1 << (s - 1)) for s in (1, 2))

        self.partner = {"outer": outer, "rows": pos[0] * 2 + 1 - core}
        self.peers = [{d: peer(s, d) for d in range(1, 8)} for s in range(2)]
        self.idx = [sum((1 - v if b else v) * (1 << s) for s, (v, b) in enumerate(zip(labels[0], _bits(d)))) for d in range(8)]
        self.grp = [[group(s, g) for g in range(4)] for s in range(2)]
        self.everyone = [self.partner, *self.peers[0].values(), *self.peers[1].values()]

    def inside(self, e):
        return pl.ds(pl.multiple_of((1 - self.low if e & 1 else self.low) * CH, CH), CH)

    def announce(self):
        for dev in self.everyone:
            pl.semaphore_signal(pltpu.get_barrier_semaphore(), inc=1, device_id=dev, device_id_type=MESH_T)

    def meet(self):
        pl.semaphore_wait(pltpu.get_barrier_semaphore(), len(self.everyone))


def gram_sum(net, meet, a, ready, o_hbm, p, o, rec0, acc0, rec1, acc1, rec2, st, s0, t0, s1, t1, s2, t2, s3, t3, s4, t4, s5, t5):
    core, partner, peers, idx, grp = net.core, net.partner, net.peers, net.idx, net.grp

    def copy(src, dst, send, recv, dev):
        return pltpu.make_async_remote_copy(src_ref=src, dst_ref=dst, send_sem=send, recv_sem=recv, device_id=dev, device_id_type=MESH_T)

    sent = []

    def go(c):
        c.start()
        sent.append(c)
        return c

    def tile(t, wait):
        lo, hi = TILES[t]

        def body(s, _):
            if wait:
                ready(s)
            at = rows_at(s)
            c = dot(a[at, :hi], a[at, lo:hi], 0, 0)
            for j in range(lo // B, hi // B):
                for i in range(j + 1):
                    h, m, quarter = PLACE[i, j]
                    c_ij = c[i * B:(i + 1) * B, j * B - lo:(j + 1) * B - lo]
                    p[h, m:m + 2, quarter] = p[h, m:m + 2, quarter] + c_ij.reshape(2, PAIR, B)
            return 0

        lax.fori_loop(0, NSTEP, body, 0)

    swap = {}

    def exchange(quarter):
        swap[quarter] = go(copy(p.at[1 - core, :, quarter], rec0.at[quarter], s0.at[quarter], t0.at[quarter], partner))

    def out1(quarter, d):
        return copy(acc0.at[quarter, idx[d]], rec1.at[quarter, d - 1], s1.at[quarter, d - 1], t1.at[quarter, d - 1], peers[0][d])

    def scatter(quarter):
        swap[quarter].wait_recv()
        acc0[quarter] = p[core, :, quarter] + rec0[quarter]
        for d in FAR_FIRST:
            go(out1(quarter, d))

    tile(TILE_ORDER[0], True)
    meet()
    exchange(0)
    for quarter in range(1, 4):
        tile(TILE_ORDER[quarter], False)
        exchange(quarter)
        scatter(quarter - 1)
    scatter(3)
    out2 = {}
    for g in (3, 2, 1, 0):
        quarter = grp[1][g]
        for d in range(1, 8):
            out1(quarter, d).wait_recv()
        total = acc0[quarter, idx[0]]
        for d in range(1, 8):
            total = total + rec1[quarter, d - 1]
        acc1[g] = total
        for e in (2 * g + 1, 2 * g):
            if e:
                out2[e] = go(copy(acc1.at[g, net.inside(e)], rec2.at[e - 1], s2.at[e - 1], t2.at[e - 1], peers[1][e]))
    for e in range(1, 8):
        out2[e].wait_recv()
    total = acc1[0, net.inside(0), :]
    for e in range(1, 8):
        total = total + rec2[e - 1]

    def chunk(e):
        return o.at[core, idx[0], grp[1][e // 2], net.inside(e)]

    o[core, idx[0], grp[1][0], net.inside(0), :] = total
    for e in FAR_FIRST:
        go(copy(chunk(0), chunk(0), s3.at[e - 1], t3.at[e - 1], peers[1][e]))
    for g in range(4):
        for e in (2 * g, 2 * g + 1):
            if e:
                copy(chunk(e), chunk(e), s3.at[e - 1], t3.at[e - 1], peers[1][e]).wait_recv()
        for d in FAR_FIRST:
            mine = o.at[core, idx[0], grp[1][g]]
            go(copy(mine, mine, s4.at[g, d - 1], t4.at[g, d - 1], peers[0][d]))
    stores = []

    def store(half, g, n):
        if o_hbm is None:
            return
        stores.append(pltpu.make_async_copy(o.at[half, :, g], o_hbm.at[half, :, g], st.at[n]))
        stores[-1].start()

    for g in range(4):
        for d in range(1, 8):
            got = o.at[core, idx[d], grp[1][g]]
            copy(got, got, s4.at[g, d - 1], t4.at[g, d - 1], peers[0][d]).wait_recv()
        whole = o.at[core, :, grp[1][g]]
        go(copy(whole, whole, s5.at[g], t5.at[g], partner))
        store(core, grp[1][g], g)
    for g in range(4):
        got = o.at[1 - core, :, grp[0][g]]
        copy(got, got, s5.at[g], t5.at[g], partner).wait_recv()
        store(1 - core, grp[0][g], 4 + g)
    for c in sent:
        c.wait_send()
    for c in stores:
        c.wait()


def sweep_one_kernel(a_hbm, q_hbm, o_hbm, r_hbm, w, xd, a, q, asem, qsem, rsem, *sums):
    net = Net()
    net.announce()
    first, second = sums[:len(sums) // 2], sums[len(sums) // 2:]

    def a_part(s):
        return pltpu.make_async_copy(a_hbm.at[rows_at(s)], a.at[rows_at(s)], asem.at[s])

    def q_part(s):
        return pltpu.make_async_copy(q.at[rows_at(s)], q_hbm.at[rows_at(s)], qsem.at[s])

    for s in range(NSTEP):
        a_part(s).start()
    for p in (first[0], second[0]):
        p[...] = jnp.zeros(SUMS, jnp.float32)
    clear(w)
    gram_sum(net, net.meet, a, lambda s: a_part(s).wait(), None, *first)
    factor(first[1], w, xd)
    keep = pltpu.make_async_copy(w.at[:, pl.ds(0, N)], r_hbm, rsem.at[0])
    keep.start()

    def body(s, _):
        solve_rows(a.at[rows_at(s)], w, q.at[rows_at(s)])
        q_part(s).start()
        return 0

    lax.fori_loop(0, NSTEP, body, 0)
    gram_sum(net, lambda: None, q, lambda s: None, o_hbm, *second)
    for s in range(NSTEP):
        q_part(s).wait()
    keep.wait()


def sweep_two_kernel(g_hbm, a_hbm, r1_hbm, q_hbm, r_hbm, g, w, xd, a, q, r1, r, sem, qsem, rsem):
    load_g = pltpu.make_async_copy(g_hbm, g, sem.at[2])
    load_g.start()
    load = pltpu.make_async_copy(a_hbm, a, sem.at[0])
    load.start()
    load_r = pltpu.make_async_copy(r1_hbm, r1, sem.at[1])
    load_r.start()
    clear(w)
    load_g.wait()
    factor(g, w, xd)
    load.wait()

    def body(s, _):
        at = rows_at(s)
        solve_rows(a.at[at], w, q.at[at])
        pltpu.make_async_copy(q.at[at], q_hbm.at[at], qsem.at[s]).start()
        return 0

    lax.fori_loop(0, NSTEP, body, 0)
    load_r.wait()
    stores = []
    for n, (lo, hi) in enumerate(TILES):
        if lo:
            r[lo:hi, :lo] = jnp.zeros((hi - lo, lo), jnp.float32)
        for clo, chi in TILES[n:]:
            r[lo:hi, clo:chi] = dot(w[lo:hi, lo:chi], r1[lo:chi, clo:chi], 1, 0)
        at = pl.ds(lo, hi - lo)
        stores.append(pltpu.make_async_copy(r.at[at], r_hbm.at[at], rsem.at[n]))
        stores[-1].start()
    for s in range(NSTEP):
        pltpu.make_async_copy(q.at[rows_at(s)], q_hbm.at[rows_at(s)], qsem.at[s]).wait()
    for c in stores:
        c.wait()


VM = pl.BlockSpec(memory_space=pltpu.VMEM)
ANY = pl.BlockSpec(memory_space=pltpu.HBM)
PARAMS = pltpu.CompilerParams(vmem_limit_bytes=63 * 2**20)
DMA = pltpu.SemaphoreType.DMA


def out(*s):
    return jax.ShapeDtypeStruct(s, jnp.float32)


def buf(*s):
    return pltpu.VMEM(s, jnp.float32)


def sum_scratch():
    sems = [DMA((8,))]
    for n in ((4,), (4, 7), (7,), (7,), (4, 7), (4,)):
        sems += [DMA(n)] * 2
    return [buf(*SUMS), buf(*SUMS), buf(4, 8, PAIR, B), buf(4, 8, PAIR, B), buf(4, 7, PAIR, B), buf(4, PAIR, B), buf(7, CH, B)] + sems


def sweep_one(a):
    return pl.pallas_call(
        sweep_one_kernel, out_shape=[out(M_LOC, N), out(*SUMS), out(N, N)], in_specs=[ANY], out_specs=[ANY, ANY, ANY],
        scratch_shapes=[buf(N, 2 * N), buf(B, B), buf(M_LOC, N), buf(M_LOC, N), DMA((NSTEP,)), DMA((NSTEP,)), DMA((1,))]
        + sum_scratch() + sum_scratch(),
        compiler_params=pltpu.CompilerParams(collective_id=0, has_side_effects=True, vmem_limit_bytes=63 * 2**20), name="sweep_one",
    )(a)


def sweep_two(g, q1, r1):
    return pl.pallas_call(
        sweep_two_kernel, out_shape=[out(M_LOC, N), out(N, N)], in_specs=[ANY, ANY, ANY], out_specs=[ANY, ANY],
        scratch_shapes=[buf(*SUMS), buf(N, 2 * N), buf(B, B), buf(M_LOC, N), buf(M_LOC, N), buf(N, N), buf(N, N), DMA((3,)), DMA((NSTEP,)), DMA((4,))],
        compiler_params=PARAMS, name="sweep_two",
    )(g, q1, r1)


def solution(mesh):
    row_spec = P(("batch", "outer", "rows"), None)

    def local_qr(a):
        q1, g2, r1 = sweep_one(a)
        return tuple(sweep_two(g2, q1, r1))

    return jax.shard_map(local_qr, mesh=mesh, in_specs=(row_spec,), out_specs=(row_spec, P("batch", None)), check_vma=False)
```

```python
import jax
import jax.numpy as jnp
from jax import lax
from jax.experimental import pallas as pl
from jax.experimental.pallas import tpu as pltpu
from jax.sharding import PartitionSpec as P

HI = lax.Precision.HIGHEST
N = 896
B = 128
NB = N // B
NG = B // 8


def dot(a, b, ca, cb):
    return lax.dot_general(a, b, (((ca,), (cb,)), ((), ())), precision=HI, preferred_element_type=jnp.float32)


def lane_col(v, c):
    lane = lax.broadcasted_iota(jnp.int32, (8, B), 1)
    return jnp.broadcast_to(jnp.sum(jnp.where(lane == c, v, 0.0), axis=1, keepdims=True), (8, B))


def sub_row(v, k):
    return jnp.broadcast_to(v[k:k + 1, :], (8, B))


def factor_diag(diag):
    sub = lax.broadcasted_iota(jnp.int32, (8, B), 0)
    lane = lax.broadcasted_iota(jnp.int32, (8, B), 1)
    m = list(diag)
    rows, inv = [None] * NG, [None] * NG
    for p in range(NG // 2):
        g0 = 16 * p
        here = (lane >= g0) & (lane < g0 + 16)
        own = m[2 * p:2 * p + 2]
        cols = [[lane_col(own[r], g0 + k) for k in range(8 * r + 8)] for r in range(2)]
        dp = list(own)
        z = [jnp.where(here, jnp.where(lane == sub + (g0 + 8 * r), 1.0, 0.0), own[r]) for r in range(2)]
        near = m[2 * p + 2:2 * p + 4]
        cq = [[lane_col(v, g0 + k) for k in range(16)] for v in near]
        mq = [jnp.where(here, 0.0, v) for v in near]
        pivs = [jnp.ones((8, B), jnp.float32)] * 2
        for k in range(16):
            rk, sk = k // 8, k % 8
            piv = sub_row(cols[rk][k], sk)
            rec = 1.0 / piv
            pivs[rk] = jnp.where(sub == sk, piv, pivs[rk])
            for kk in range(k + 1, 16):
                t = sub_row(cols[kk // 8][k], kk % 8) * rec
                for r in range(kk // 8, 2):
                    cols[r][kk] = cols[r][kk] - cols[r][k] * t
                for c in cq:
                    c[kk] = c[kk] - c[k] * t
            v = sub_row(z[rk], sk) * rec
            y = sub_row(dp[rk], sk) * rec
            for r in range(rk, 2):
                low = jnp.where(sub > sk, cols[r][k], 0.0) if r == rk else cols[r][k]
                z[r] = z[r] - low * v
                dp[r] = dp[r] - low * y
            for n, c in enumerate(cq):
                mq[n] = mq[n] - c[k] * v
        scaled = []
        for r in range(2):
            scale = lax.rsqrt(pivs[r])
            scaled.append(z[r] * scale)
            rows[2 * p + r] = jnp.where(lane >= sub + (g0 + 8 * r), dp[r] * scale, 0.0)
            inv[2 * p + r] = jnp.where(lane < g0 + 16, scaled[r], 0.0)
        if 2 * p + 4 < NG:
            both = jnp.concatenate(scaled, axis=0)
            upd = dot(both, both, 0, 0)
            for q in range(2 * p + 4, NG):
                m[q] = jnp.where(here, 0.0, m[q]) - upd[8 * q:8 * q + 8, :]
        for n, v in enumerate(mq):
            m[2 * p + 2 + n] = v
    return rows, inv


TILES = [(lo, min(lo + 256, N)) for lo in range(0, N, 256)]
TILE_ORDER = (3, 1, 2, 0)
CH = 32
PAIR = 2 * CH
SUMS = (2, 8, 4, PAIR, B)


def _places():
    blocks = [(i, j) for t in TILE_ORDER for j in range(TILES[t][0] // B, TILES[t][1] // B) for i in range(j + 1)]
    return {b: (n % 7 // 4, n % 7 % 4 * 2, n // 7) for n, b in enumerate(blocks)}


PLACE = _places()


def read_block(g_ref, i, j):
    h, m, quarter = PLACE[i, j]
    return g_ref[h, m:m + 2, quarter].reshape(B, B)


def mult(x):
    return pl.multiple_of(x, B)


def clear(w):
    w[:, N:] = jnp.zeros((N, N), jnp.float32)
    for i in range(1, NB):
        w[i * B:(i + 1) * B, :i * B] = jnp.zeros((B, i * B), jnp.float32)


def factor(g_ref, w, xd):
    for i in range(NB):
        for j in range(i, NB):
            w[i * B:(i + 1) * B, j * B:(j + 1) * B] = read_block(g_ref, i, j)

    def step(j, _):
        r0 = mult(j * B)
        rr = pl.ds(r0, B)
        group = [pl.ds(pl.multiple_of(r0 + 8 * q, 8), 8) for q in range(NG)]
        rows, inv = factor_diag([w[gq, pl.ds(r0, B)] for gq in group])
        for q in range(NG):
            w[group[q], pl.ds(r0, B)] = rows[q]
            w[group[q], pl.ds(mult(r0 + N), B)] = inv[q]
            xd[pl.ds(8 * q, 8), :] = inv[q]
        mid = pl.ds(mult(r0 + B), N - B)
        w[rr, mid] = dot(xd[...], w[rr, mid], 1, 0)
        odd = j % 2

        def trail(top, depth, first, count):
            src = pl.ds(mult(top), depth)
            win = pl.ds(mult(top + depth), N)

            def body(i, _):
                ri = pl.ds(mult((first + count * i) * B), count * B)
                w[ri, win] = w[ri, win] - dot(w[src, ri], w[src, win], 0, 0)
                return 0

            return body

        lax.fori_loop(0, jnp.where(odd == 0, jnp.minimum(NB - 1 - j, 1), 0), trail(r0, B, j + 1, 1), 0)
        before = jnp.maximum(r0 - B, 0)
        lax.fori_loop(0, odd, trail(before, 2 * B, j + 1, 1), 0)
        lax.fori_loop(0, jnp.where(odd == 1, (NB - 2 - j) // 2, 0), trail(before, 2 * B, j + 2, 2), 0)
        return 0

    lax.fori_loop(0, NB, step, 0)
    for i in range(1, NB):
        w[i * B:(i + 1) * B, :i * B] = jnp.zeros((B, i * B), jnp.float32)


M_LOC = 1024
STEP = 256
NSTEP = M_LOC // STEP


def solve_rows(a, w, q):
    for lo, hi in TILES:
        q[:, lo:hi] = dot(a[:, :hi], w[lo:hi, N:N + hi], 1, 1)


def rows_at(s):
    return pl.ds(pl.multiple_of(s * STEP, STEP), STEP)


MESH_T = pl.DeviceIdType.MESH
FAR_FIRST = (7, 3, 5, 6, 1, 2, 4)


def _bits(d):
    return tuple((d >> s) & 1 for s in range(3))


def _flip(v, kind):
    return (1 - kind) * (v + 1 - 2 * (v % 2)) + kind * (3 - v)


def _label(v, kind):
    return (1 - kind) * ((v % 2 + v // 2) % 2) + kind * (v // 2)


class Net:
    def __init__(self):
        outer, row = lax.axis_index("outer"), lax.axis_index("rows")
        pos = (row // 2, outer % 4, outer // 4)
        self.core = core = row % 2
        kinds = (core, 1 - core)
        labels = [tuple(_label(v, k) for v in pos) for k in kinds]
        self.low = labels[1][0]

        def peer(stage, d):
            x, y, z = (_flip(v, kinds[stage]) if b else v for v, b in zip(pos, _bits(d)))
            return {"outer": z * 4 + y, "rows": x * 2 + core}

        def group(stage, g):
            return sum((1 - labels[stage][s] if (g >> (s - 1)) & 1 else labels[stage][s]) * (1 << (s - 1)) for s in (1, 2))

        self.partner = {"outer": outer, "rows": pos[0] * 2 + 1 - core}
        self.peers = [{d: peer(s, d) for d in range(1, 8)} for s in range(2)]
        self.idx = [sum((1 - v if b else v) * (1 << s) for s, (v, b) in enumerate(zip(labels[0], _bits(d)))) for d in range(8)]
        self.grp = [[group(s, g) for g in range(4)] for s in range(2)]
        self.everyone = [self.partner, *self.peers[0].values(), *self.peers[1].values()]

    def inside(self, e):
        return pl.ds(pl.multiple_of((1 - self.low if e & 1 else self.low) * CH, CH), CH)

    def announce(self):
        for dev in self.everyone:
            pl.semaphore_signal(pltpu.get_barrier_semaphore(), inc=1, device_id=dev, device_id_type=MESH_T)

    def meet(self):
        pl.semaphore_wait(pltpu.get_barrier_semaphore(), len(self.everyone))


def gram_sum(net, meet, a, ready, o_hbm, p, o, rec0, acc0, rec1, acc1, rec2, st, s0, t0, s1, t1, s2, t2, s3, t3, s4, t4, s5, t5):
    core, partner, peers, idx, grp = net.core, net.partner, net.peers, net.idx, net.grp

    def copy(src, dst, send, recv, dev):
        return pltpu.make_async_remote_copy(src_ref=src, dst_ref=dst, send_sem=send, recv_sem=recv, device_id=dev, device_id_type=MESH_T)

    sent = []

    def go(c):
        c.start()
        sent.append(c)
        return c

    def tile(t, wait):
        lo, hi = TILES[t]

        def body(s, _):
            if wait:
                ready(s)
            at = rows_at(s)
            c = dot(a[at, :hi], a[at, lo:hi], 0, 0)
            for j in range(lo // B, hi // B):
                for i in range(j + 1):
                    h, m, quarter = PLACE[i, j]
                    c_ij = c[i * B:(i + 1) * B, j * B - lo:(j + 1) * B - lo]
                    p[h, m:m + 2, quarter] = p[h, m:m + 2, quarter] + c_ij.reshape(2, PAIR, B)
            return 0

        lax.fori_loop(0, NSTEP, body, 0)

    swap = {}

    def exchange(quarter):
        swap[quarter] = go(copy(p.at[1 - core, :, quarter], rec0.at[quarter], s0.at[quarter], t0.at[quarter], partner))

    def out1(quarter, d):
        return copy(acc0.at[quarter, idx[d]], rec1.at[quarter, d - 1], s1.at[quarter, d - 1], t1.at[quarter, d - 1], peers[0][d])

    def scatter(quarter):
        swap[quarter].wait_recv()
        acc0[quarter] = p[core, :, quarter] + rec0[quarter]
        for d in FAR_FIRST:
            go(out1(quarter, d))

    tile(TILE_ORDER[0], True)
    meet()
    exchange(0)
    for quarter in range(1, 4):
        tile(TILE_ORDER[quarter], False)
        exchange(quarter)
        scatter(quarter - 1)
    scatter(3)
    out2 = {}
    for g in (3, 2, 1, 0):
        quarter = grp[1][g]
        for d in range(1, 8):
            out1(quarter, d).wait_recv()
        total = acc0[quarter, idx[0]]
        for d in range(1, 8):
            total = total + rec1[quarter, d - 1]
        acc1[g] = total
        for e in (2 * g + 1, 2 * g):
            if e:
                out2[e] = go(copy(acc1.at[g, net.inside(e)], rec2.at[e - 1], s2.at[e - 1], t2.at[e - 1], peers[1][e]))
    for e in range(1, 8):
        out2[e].wait_recv()
    total = acc1[0, net.inside(0), :]
    for e in range(1, 8):
        total = total + rec2[e - 1]

    def chunk(e):
        return o.at[core, idx[0], grp[1][e // 2], net.inside(e)]

    o[core, idx[0], grp[1][0], net.inside(0), :] = total
    for e in FAR_FIRST:
        go(copy(chunk(0), chunk(0), s3.at[e - 1], t3.at[e - 1], peers[1][e]))
    for g in range(4):
        for e in (2 * g, 2 * g + 1):
            if e:
                copy(chunk(e), chunk(e), s3.at[e - 1], t3.at[e - 1], peers[1][e]).wait_recv()
        for d in FAR_FIRST:
            mine = o.at[core, idx[0], grp[1][g]]
            go(copy(mine, mine, s4.at[g, d - 1], t4.at[g, d - 1], peers[0][d]))
    stores = []

    def store(half, g, n):
        if o_hbm is None:
            return
        stores.append(pltpu.make_async_copy(o.at[half, :, g], o_hbm.at[half, :, g], st.at[n]))
        stores[-1].start()

    for g in range(4):
        for d in range(1, 8):
            got = o.at[core, idx[d], grp[1][g]]
            copy(got, got, s4.at[g, d - 1], t4.at[g, d - 1], peers[0][d]).wait_recv()
        whole = o.at[core, :, grp[1][g]]
        go(copy(whole, whole, s5.at[g], t5.at[g], partner))
        store(core, grp[1][g], g)
    for g in range(4):
        got = o.at[1 - core, :, grp[0][g]]
        copy(got, got, s5.at[g], t5.at[g], partner).wait_recv()
        store(1 - core, grp[0][g], 4 + g)
    for c in sent:
        c.wait_send()
    for c in stores:
        c.wait()


def sweep_one_kernel(a_hbm, q_hbm, o_hbm, r_hbm, w, xd, a, q, asem, qsem, rsem, *sums):
    net = Net()
    net.announce()
    first, second = sums[:len(sums) // 2], sums[len(sums) // 2:]

    def a_part(s):
        return pltpu.make_async_copy(a_hbm.at[rows_at(s)], a.at[rows_at(s)], asem.at[s])

    def q_part(s):
        return pltpu.make_async_copy(q.at[rows_at(s)], q_hbm.at[rows_at(s)], qsem.at[s])

    for s in range(NSTEP):
        a_part(s).start()
    for p in (first[0], second[0]):
        p[...] = jnp.zeros(SUMS, jnp.float32)
    clear(w)
    gram_sum(net, net.meet, a, lambda s: a_part(s).wait(), None, *first)
    factor(first[1], w, xd)
    keep = pltpu.make_async_copy(w.at[:, pl.ds(0, N)], r_hbm, rsem.at[0])
    keep.start()

    def body(s, _):
        solve_rows(a.at[rows_at(s)], w, q.at[rows_at(s)])
        q_part(s).start()
        return 0

    lax.fori_loop(0, NSTEP, body, 0)
    gram_sum(net, lambda: None, q, lambda s: None, o_hbm, *second)
    for s in range(NSTEP):
        q_part(s).wait()
    keep.wait()


def sweep_two_kernel(g_hbm, a_hbm, r1_hbm, q_hbm, r_hbm, g, w, xd, a, q, r1, r, sem, qsem, rsem):
    load_g = pltpu.make_async_copy(g_hbm, g, sem.at[2])
    load_g.start()
    load = pltpu.make_async_copy(a_hbm, a, sem.at[0])
    load.start()
    load_r = pltpu.make_async_copy(r1_hbm, r1, sem.at[1])
    load_r.start()
    clear(w)
    load_g.wait()
    factor(g, w, xd)
    load.wait()

    def body(s, _):
        at = rows_at(s)
        solve_rows(a.at[at], w, q.at[at])
        pltpu.make_async_copy(q.at[at], q_hbm.at[at], qsem.at[s]).start()
        return 0

    lax.fori_loop(0, NSTEP, body, 0)
    load_r.wait()
    stores = []
    for n, (lo, hi) in enumerate(TILES):
        if lo:
            r[lo:hi, :lo] = jnp.zeros((hi - lo, lo), jnp.float32)
        for clo, chi in TILES[n:]:
            r[lo:hi, clo:chi] = dot(w[lo:hi, lo:chi], r1[lo:chi, clo:chi], 1, 0)
        at = pl.ds(lo, hi - lo)
        stores.append(pltpu.make_async_copy(r.at[at], r_hbm.at[at], rsem.at[n]))
        stores[-1].start()
    for s in range(NSTEP):
        pltpu.make_async_copy(q.at[rows_at(s)], q_hbm.at[rows_at(s)], qsem.at[s]).wait()
    for c in stores:
        c.wait()


VM = pl.BlockSpec(memory_space=pltpu.VMEM)
ANY = pl.BlockSpec(memory_space=pltpu.HBM)
PARAMS = pltpu.CompilerParams(vmem_limit_bytes=63 * 2**20)
DMA = pltpu.SemaphoreType.DMA


def out(*s):
    return jax.ShapeDtypeStruct(s, jnp.float32)


def buf(*s):
    return pltpu.VMEM(s, jnp.float32)


def sum_scratch():
    sems = [DMA((8,))]
    for n in ((4,), (4, 7), (7,), (7,), (4, 7), (4,)):
        sems += [DMA(n)] * 2
    return [buf(*SUMS), buf(*SUMS), buf(4, 8, PAIR, B), buf(4, 8, PAIR, B), buf(4, 7, PAIR, B), buf(4, PAIR, B), buf(7, CH, B)] + sems


def sweep_one(a):
    return pl.pallas_call(
        sweep_one_kernel, out_shape=[out(M_LOC, N), out(*SUMS), out(N, N)], in_specs=[ANY], out_specs=[ANY, ANY, ANY],
        scratch_shapes=[buf(N, 2 * N), buf(B, B), buf(M_LOC, N), buf(M_LOC, N), DMA((NSTEP,)), DMA((NSTEP,)), DMA((1,))]
        + sum_scratch() + sum_scratch(),
        compiler_params=pltpu.CompilerParams(collective_id=0, has_side_effects=True, vmem_limit_bytes=63 * 2**20), name="sweep_one",
    )(a)


def sweep_two(g, q1, r1):
    return pl.pallas_call(
        sweep_two_kernel, out_shape=[out(M_LOC, N), out(N, N)], in_specs=[ANY, ANY, ANY], out_specs=[ANY, ANY],
        scratch_shapes=[buf(*SUMS), buf(N, 2 * N), buf(B, B), buf(M_LOC, N), buf(M_LOC, N), buf(N, N), buf(N, N), DMA((3,)), DMA((NSTEP,)), DMA((4,))],
        compiler_params=PARAMS, name="sweep_two",
    )(g, q1, r1)


def solution(mesh):
    row_spec = P(("batch", "outer", "rows"), None)

    def local_qr(a):
        q1, g2, r1 = sweep_one(a)
        return tuple(sweep_two(g2, q1, r1))

    return jax.shard_map(local_qr, mesh=mesh, in_specs=(row_spec,), out_specs=(row_spec, P("batch", None)), check_vma=False)
```

```python
import jax
import jax.numpy as jnp
from jax import lax
from jax.experimental import pallas as pl
from jax.experimental.pallas import tpu as pltpu
from jax.sharding import PartitionSpec as P

HI = lax.Precision.HIGHEST
N = 896
B = 128
NB = N // B
NG = B // 8


def dot(a, b, ca, cb):
    return lax.dot_general(a, b, (((ca,), (cb,)), ((), ())), precision=HI, preferred_element_type=jnp.float32)


def lane_col(v, c):
    lane = lax.broadcasted_iota(jnp.int32, (8, B), 1)
    return jnp.broadcast_to(jnp.sum(jnp.where(lane == c, v, 0.0), axis=1, keepdims=True), (8, B))


def sub_row(v, k):
    return jnp.broadcast_to(v[k:k + 1, :], (8, B))


def factor_diag(diag):
    sub = lax.broadcasted_iota(jnp.int32, (8, B), 0)
    lane = lax.broadcasted_iota(jnp.int32, (8, B), 1)
    m = list(diag)
    rows, inv = [None] * NG, [None] * NG
    for p in range(NG // 2):
        g0 = 16 * p
        here = (lane >= g0) & (lane < g0 + 16)
        own = m[2 * p:2 * p + 2]
        cols = [[lane_col(own[r], g0 + k) for k in range(8 * r + 8)] for r in range(2)]
        dp = list(own)
        z = [jnp.where(here, jnp.where(lane == sub + (g0 + 8 * r), 1.0, 0.0), own[r]) for r in range(2)]
        near = m[2 * p + 2:2 * p + 4]
        cq = [[lane_col(v, g0 + k) for k in range(16)] for v in near]
        mq = [jnp.where(here, 0.0, v) for v in near]
        pivs = [jnp.ones((8, B), jnp.float32)] * 2
        for k in range(16):
            rk, sk = k // 8, k % 8
            piv = sub_row(cols[rk][k], sk)
            rec = 1.0 / piv
            pivs[rk] = jnp.where(sub == sk, piv, pivs[rk])
            for kk in range(k + 1, 16):
                t = sub_row(cols[kk // 8][k], kk % 8) * rec
                for r in range(kk // 8, 2):
                    cols[r][kk] = cols[r][kk] - cols[r][k] * t
                for c in cq:
                    c[kk] = c[kk] - c[k] * t
            v = sub_row(z[rk], sk) * rec
            y = sub_row(dp[rk], sk) * rec
            for r in range(rk, 2):
                low = jnp.where(sub > sk, cols[r][k], 0.0) if r == rk else cols[r][k]
                z[r] = z[r] - low * v
                dp[r] = dp[r] - low * y
            for n, c in enumerate(cq):
                mq[n] = mq[n] - c[k] * v
        scaled = []
        for r in range(2):
            scale = lax.rsqrt(pivs[r])
            scaled.append(z[r] * scale)
            rows[2 * p + r] = jnp.where(lane >= sub + (g0 + 8 * r), dp[r] * scale, 0.0)
            inv[2 * p + r] = jnp.where(lane < g0 + 16, scaled[r], 0.0)
        if 2 * p + 4 < NG:
            both = jnp.concatenate(scaled, axis=0)
            upd = dot(both, both, 0, 0)
            for q in range(2 * p + 4, NG):
                m[q] = jnp.where(here, 0.0, m[q]) - upd[8 * q:8 * q + 8, :]
        for n, v in enumerate(mq):
            m[2 * p + 2 + n] = v
    return rows, inv


TILES = [(lo, min(lo + 256, N)) for lo in range(0, N, 256)]
TILE_ORDER = (3, 1, 2, 0)
CH = 32
PAIR = 2 * CH
SUMS = (2, 8, 4, PAIR, B)


def _places():
    blocks = [(i, j) for t in TILE_ORDER for j in range(TILES[t][0] // B, TILES[t][1] // B) for i in range(j + 1)]
    return {b: (n % 7 // 4, n % 7 % 4 * 2, n // 7) for n, b in enumerate(blocks)}


PLACE = _places()


def read_block(g_ref, i, j):
    h, m, quarter = PLACE[i, j]
    return g_ref[h, m:m + 2, quarter].reshape(B, B)


def mult(x):
    return pl.multiple_of(x, B)


def clear(w):
    w[:, N:] = jnp.zeros((N, N), jnp.float32)
    for i in range(1, NB):
        w[i * B:(i + 1) * B, :i * B] = jnp.zeros((B, i * B), jnp.float32)


def factor(g_ref, w, xd):
    for i in range(NB):
        for j in range(i, NB):
            w[i * B:(i + 1) * B, j * B:(j + 1) * B] = read_block(g_ref, i, j)

    def step(j, _):
        r0 = mult(j * B)
        rr = pl.ds(r0, B)
        group = [pl.ds(pl.multiple_of(r0 + 8 * q, 8), 8) for q in range(NG)]
        rows, inv = factor_diag([w[gq, pl.ds(r0, B)] for gq in group])
        for q in range(NG):
            w[group[q], pl.ds(r0, B)] = rows[q]
            w[group[q], pl.ds(mult(r0 + N), B)] = inv[q]
            xd[pl.ds(8 * q, 8), :] = inv[q]
        mid = pl.ds(mult(r0 + B), N - B)
        w[rr, mid] = dot(xd[...], w[rr, mid], 1, 0)
        odd = j % 2

        def trail(top, depth, first, count):
            src = pl.ds(mult(top), depth)
            win = pl.ds(mult(top + depth), N)

            def body(i, _):
                ri = pl.ds(mult((first + count * i) * B), count * B)
                w[ri, win] = w[ri, win] - dot(w[src, ri], w[src, win], 0, 0)
                return 0

            return body

        lax.fori_loop(0, jnp.where(odd == 0, jnp.minimum(NB - 1 - j, 1), 0), trail(r0, B, j + 1, 1), 0)
        before = jnp.maximum(r0 - B, 0)
        lax.fori_loop(0, odd, trail(before, 2 * B, j + 1, 1), 0)
        lax.fori_loop(0, jnp.where(odd == 1, (NB - 2 - j) // 2, 0), trail(before, 2 * B, j + 2, 2), 0)
        return 0

    lax.fori_loop(0, NB, step, 0)
    for i in range(1, NB):
        w[i * B:(i + 1) * B, :i * B] = jnp.zeros((B, i * B), jnp.float32)


M_LOC = 1024
STEP = 256
NSTEP = M_LOC // STEP


def solve_rows(a, w, q):
    for lo, hi in TILES:
        q[:, lo:hi] = dot(a[:, :hi], w[lo:hi, N:N + hi], 1, 1)


def rows_at(s):
    return pl.ds(pl.multiple_of(s * STEP, STEP), STEP)


MESH_T = pl.DeviceIdType.MESH
FAR_FIRST = (7, 3, 5, 6, 1, 2, 4)


def _bits(d):
    return tuple((d >> s) & 1 for s in range(3))


def _flip(v, kind):
    return (1 - kind) * (v + 1 - 2 * (v % 2)) + kind * (3 - v)


def _label(v, kind):
    return (1 - kind) * ((v % 2 + v // 2) % 2) + kind * (v // 2)


class Net:
    def __init__(self):
        outer, row = lax.axis_index("outer"), lax.axis_index("rows")
        pos = (row // 2, outer % 4, outer // 4)
        self.core = core = row % 2
        kinds = (core, 1 - core)
        labels = [tuple(_label(v, k) for v in pos) for k in kinds]
        self.own = sum(v * (1 << s) for s, v in enumerate(labels[1]))

        def peer(stage, d):
            x, y, z = (_flip(v, kinds[stage]) if b else v for v, b in zip(pos, _bits(d)))
            return {"outer": z * 4 + y, "rows": x * 2 + core}

        self.partner = {"outer": outer, "rows": pos[0] * 2 + 1 - core}
        self.peers = [{d: peer(s, d) for d in range(1, 8)} for s in range(2)]
        self.idx = [sum((1 - v if b else v) * (1 << s) for s, (v, b) in enumerate(zip(labels[0], _bits(d)))) for d in range(8)]
        self.everyone = [self.partner, *self.peers[0].values(), *self.peers[1].values()]

    def announce(self):
        for dev in self.everyone:
            pl.semaphore_signal(pltpu.get_barrier_semaphore(), inc=1, device_id=dev, device_id_type=MESH_T)

    def meet(self):
        pl.semaphore_wait(pltpu.get_barrier_semaphore(), len(self.everyone))


def gram_sum(net, meet, a, ready, o_hbm, p, o, rec0, acc0, rec1, rec2, st, s0, t0, s1, t1, s2, t2, s3, t3, s4, t4):
    core, partner, peers, idx = net.core, net.partner, net.peers, net.idx

    def copy(src, dst, send, recv, dev):
        return pltpu.make_async_remote_copy(src_ref=src, dst_ref=dst, send_sem=send, recv_sem=recv, device_id=dev, device_id_type=MESH_T)

    sent = []

    def go(c):
        c.start()
        sent.append(c)
        return c

    def tile(t, wait):
        lo, hi = TILES[t]

        def body(s, _):
            if wait:
                ready(s)
            at = rows_at(s)
            c = dot(a[at, :hi], a[at, lo:hi], 0, 0)
            for j in range(lo // B, hi // B):
                for i in range(j + 1):
                    h, m, quarter = PLACE[i, j]
                    c_ij = c[i * B:(i + 1) * B, j * B - lo:(j + 1) * B - lo]
                    p[h, m:m + 2, quarter] = p[h, m:m + 2, quarter] + c_ij.reshape(2, PAIR, B)
            return 0

        lax.fori_loop(0, NSTEP, body, 0)

    swap = {}

    def exchange(quarter):
        swap[quarter] = go(copy(p.at[1 - core, :, quarter], rec0.at[quarter], s0.at[quarter], t0.at[quarter], partner))

    def out1(quarter, d):
        return copy(acc0.at[quarter, idx[d]], rec1.at[quarter, d - 1], s1.at[quarter, d - 1], t1.at[quarter, d - 1], peers[0][d])

    def scatter(quarter):
        swap[quarter].wait_recv()
        acc0[quarter] = p[core, :, quarter] + rec0[quarter]
        for d in FAR_FIRST:
            go(out1(quarter, d))

    tile(TILE_ORDER[0], True)
    meet()
    exchange(0)
    for quarter in range(1, 4):
        tile(TILE_ORDER[quarter], False)
        exchange(quarter)
        scatter(quarter - 1)
    scatter(3)
    here = net.own

    def out2(quarter, e):
        return copy(rec2.at[quarter, here], rec2.at[quarter, here], s2.at[quarter, e - 1], t2.at[quarter, e - 1], peers[1][e])

    def spread(quarter):
        for d in range(1, 8):
            out1(quarter, d).wait_recv()
        total = acc0[quarter, idx[0]]
        for d in range(1, 8):
            total = total + rec1[quarter, d - 1]
        rec2[quarter, here] = total
        for e in FAR_FIRST:
            go(out2(quarter, e))

    def back(quarter, d, owner):
        at = o.at[core, owner, quarter]
        return copy(at, at, s3.at[quarter, d - 1], t3.at[quarter, d - 1], peers[0][d])

    def finish(quarter):
        for e in range(1, 8):
            out2(quarter, e).wait_recv()
        total = rec2[quarter, 0]
        for n in range(1, 8):
            total = total + rec2[quarter, n]
        o[core, idx[0], quarter] = total
        for d in FAR_FIRST:
            go(back(quarter, d, idx[0]))

    stores = []

    def store(half, quarter, n):
        if o_hbm is None:
            return
        stores.append(pltpu.make_async_copy(o.at[half, :, quarter], o_hbm.at[half, :, quarter], st.at[n]))
        stores[-1].start()

    def over(half, quarter):
        at = o.at[half, :, quarter]
        return copy(at, at, s4.at[quarter], t4.at[quarter], partner)

    def gather(quarter):
        for d in range(1, 8):
            back(quarter, d, idx[d]).wait_recv()
        go(over(core, quarter))
        store(core, quarter, quarter)

    spread(0)
    spread(1)
    spread(2)
    finish(0)
    spread(3)
    finish(1)
    finish(2)
    gather(0)
    finish(3)
    for quarter in range(1, 4):
        gather(quarter)
    for quarter in range(4):
        over(1 - core, quarter).wait_recv()
        store(1 - core, quarter, 4 + quarter)
    for c in sent:
        c.wait_send()
    for c in stores:
        c.wait()


def sweep_one_kernel(a_hbm, q_hbm, o_hbm, r_hbm, w, xd, a, q, asem, qsem, rsem, *sums):
    net = Net()
    net.announce()
    first, second = sums[:len(sums) // 2], sums[len(sums) // 2:]

    def a_part(s):
        return pltpu.make_async_copy(a_hbm.at[rows_at(s)], a.at[rows_at(s)], asem.at[s])

    def q_part(s):
        return pltpu.make_async_copy(q.at[rows_at(s)], q_hbm.at[rows_at(s)], qsem.at[s])

    for s in range(NSTEP):
        a_part(s).start()
    for p in (first[0], second[0]):
        p[...] = jnp.zeros(SUMS, jnp.float32)
    clear(w)
    gram_sum(net, net.meet, a, lambda s: a_part(s).wait(), None, *first)
    factor(first[1], w, xd)
    keep = pltpu.make_async_copy(w.at[:, pl.ds(0, N)], r_hbm, rsem.at[0])
    keep.start()

    def body(s, _):
        solve_rows(a.at[rows_at(s)], w, q.at[rows_at(s)])
        q_part(s).start()
        return 0

    lax.fori_loop(0, NSTEP, body, 0)
    gram_sum(net, lambda: None, q, lambda s: None, o_hbm, *second)
    for s in range(NSTEP):
        q_part(s).wait()
    keep.wait()


def sweep_two_kernel(g_hbm, a_hbm, r1_hbm, q_hbm, r_hbm, g, w, xd, a, q, r1, r, sem, qsem, rsem):
    load_g = pltpu.make_async_copy(g_hbm, g, sem.at[2])
    load_g.start()
    load = pltpu.make_async_copy(a_hbm, a, sem.at[0])
    load.start()
    load_r = pltpu.make_async_copy(r1_hbm, r1, sem.at[1])
    load_r.start()
    clear(w)
    load_g.wait()
    factor(g, w, xd)
    load.wait()

    def body(s, _):
        at = rows_at(s)
        solve_rows(a.at[at], w, q.at[at])
        pltpu.make_async_copy(q.at[at], q_hbm.at[at], qsem.at[s]).start()
        return 0

    lax.fori_loop(0, NSTEP, body, 0)
    load_r.wait()
    stores = []
    for n, (lo, hi) in enumerate(TILES):
        if lo:
            r[lo:hi, :lo] = jnp.zeros((hi - lo, lo), jnp.float32)
        for clo, chi in TILES[n:]:
            r[lo:hi, clo:chi] = dot(w[lo:hi, lo:chi], r1[lo:chi, clo:chi], 1, 0)
        at = pl.ds(lo, hi - lo)
        stores.append(pltpu.make_async_copy(r.at[at], r_hbm.at[at], rsem.at[n]))
        stores[-1].start()
    for s in range(NSTEP):
        pltpu.make_async_copy(q.at[rows_at(s)], q_hbm.at[rows_at(s)], qsem.at[s]).wait()
    for c in stores:
        c.wait()


VM = pl.BlockSpec(memory_space=pltpu.VMEM)
ANY = pl.BlockSpec(memory_space=pltpu.HBM)
PARAMS = pltpu.CompilerParams(vmem_limit_bytes=63 * 2**20)
DMA = pltpu.SemaphoreType.DMA


def out(*s):
    return jax.ShapeDtypeStruct(s, jnp.float32)


def buf(*s):
    return pltpu.VMEM(s, jnp.float32)


def sum_scratch():
    sems = [DMA((8,))]
    for n in ((4,), (4, 7), (4, 7), (4, 7), (4,)):
        sems += [DMA(n)] * 2
    return [buf(*SUMS), buf(*SUMS), buf(4, 8, PAIR, B), buf(4, 8, PAIR, B), buf(4, 7, PAIR, B), buf(4, 8, PAIR, B)] + sems


def sweep_one(a):
    return pl.pallas_call(
        sweep_one_kernel, out_shape=[out(M_LOC, N), out(*SUMS), out(N, N)], in_specs=[ANY], out_specs=[ANY, ANY, ANY],
        scratch_shapes=[buf(N, 2 * N), buf(B, B), buf(M_LOC, N), buf(M_LOC, N), DMA((NSTEP,)), DMA((NSTEP,)), DMA((1,))]
        + sum_scratch() + sum_scratch(),
        compiler_params=pltpu.CompilerParams(collective_id=0, has_side_effects=True, vmem_limit_bytes=63 * 2**20), name="sweep_one",
    )(a)


def sweep_two(g, q1, r1):
    return pl.pallas_call(
        sweep_two_kernel, out_shape=[out(M_LOC, N), out(N, N)], in_specs=[ANY, ANY, ANY], out_specs=[ANY, ANY],
        scratch_shapes=[buf(*SUMS), buf(N, 2 * N), buf(B, B), buf(M_LOC, N), buf(M_LOC, N), buf(N, N), buf(N, N), DMA((3,)), DMA((NSTEP,)), DMA((4,))],
        compiler_params=PARAMS, name="sweep_two",
    )(g, q1, r1)


def solution(mesh):
    row_spec = P(("batch", "outer", "rows"), None)

    def local_qr(a):
        q1, g2, r1 = sweep_one(a)
        return tuple(sweep_two(g2, q1, r1))

    return jax.shard_map(local_qr, mesh=mesh, in_specs=(row_spec,), out_specs=(row_spec, P("batch", None)), check_vma=False)
```
